128 devices in a mesh: gx: 8 (over y, core), gy: 16 (over z, x).
Axes of the slice: x: 4, y: 4, z: 4, core: 2. Of those that a mesh axis runs over, the one named last changes fastest.
Arguments:
- fluid_state: float32 [4, 64, 256, 256], P(None, 'gx', 'gy'), may hold values from -3 to 3
- node_disp: float32 [3, 524288], P(None, ('gx', 'gy')), may hold values from -0.02 to 0.02
- node_vel: float32 [3, 524288], P(None, ('gx', 'gy')), may hold values from -1 to 1
- fiber_angles: float32 [2, 65536], P(None, ('gx', 'gy')), may hold values from -3.140625 to 3.140625
- connectivity: int32 [27, 65536], P(None, ('gx', 'gy')), may hold values from 0 to 4095
- send_blocks: int32 [128, 128, 4], P(('gx', 'gy')), may hold values from 0 to 256, as said below
- interp_slots: int32 [4, 4096], P(None, ('gx', 'gy')), may hold values from 0 to 511, as said below
- weight_index: int32 [4, 4096], P(None, ('gx', 'gy')), may hold values from 0 to 127
- share_nodes: int32 [128, 128, 16], P(('gx', 'gy')), may hold values from 0 to 4096, as said below
- weight_table: bfloat16 [128, 128, 128], replicated, may hold values from -0.25 to 0.25
Outputs:
- fluid_out: float32 [4, 64, 256, 256], P(None, 'gx', 'gy')
- disp_out: float32 [3, 524288], P(None, ('gx', 'gy'))
- vel_out: float32 [3, 524288], P(None, ('gx', 'gy'))
The draws below stay inside these ranges and needn't reach their ends.
Inputs may be any that keep to these rules, and one draw needn't show every extreme that they name: `send_blocks`: entry [s, d, j] is the block of tile s in its j-th slot to part d; 256 marks an empty slot; in each [s, d] the filled slots come first, and some [s, d] are full. `interp_slots`: column p * 32 + b names slots of part p's received buffer, counted as source tile times 4 plus slot. `share_nodes`: entry [p, q, j] is the node of part p paired with node [q, p, j] of part q; 4096 marks an unused slot, unused on both sides together; [p, p] holds only unused slots; used slots come first.
All inputs are finite; a program needn't handle non-finite values.
Results may differ from the reference program's by a relative error of at most 0.0046.
Values may be sent and summed in bfloat16 or wider, within the bound.
No kernel may reach another device: no remote copies, remote signals or barrier semaphores. Data moves between devices by JAX's collectives and lax.ppermute only.
A program may use at most 128 MiB of HBM per device.

```python
import math
import jax
import jax.numpy as jnp
import numpy as np
from jax import lax

CX = 8
CY = 16
NZ = 256
ELEM_DEV = 512
STEPS = 3
K = 4
CAP = 4
SH = 16
WTAB = 128
NX = 64
NY = 256
FB = 256
NODES_DEV = 4096
NB = 32
ELEMS = 65536
NODES = 524288
NBLK = 4096
N_GX = 8
N_GY = 16
DEVICES = 128


def slot_counts(key):
    base = jax.random.fold_in(key, 7)
    raw = jax.random.randint(jax.random.fold_in(base, 1), (DEVICES, DEVICES), 0, 3)
    factor = jax.random.randint(jax.random.fold_in(base, 2), (1, DEVICES), 1, 4)
    counts = jnp.minimum(raw * factor, CAP)
    source = jnp.arange(DEVICES)[:, None]
    target = jnp.arange(DEVICES)[None, :]
    counts = jnp.where(source == target, CAP, counts)
    counts = jnp.where(target == (source + 1) % DEVICES, CAP, counts)
    counts = jnp.where(target == (source + DEVICES // 2) % DEVICES, CAP, counts)
    return counts


def draw_send_blocks(key, part):
    counts = slot_counts(key)
    chosen = jax.random.randint(jax.random.fold_in(key, 11), (DEVICES, DEVICES, CAP), 0, FB)
    live = jnp.arange(CAP)[None, None, :] < counts[:, :, None]
    return jnp.where(live, chosen, FB).astype(jnp.int32)


def draw_interp_slots(key, part):
    counts = slot_counts(key)
    owner = jnp.arange(NB * DEVICES) // NB
    source = jax.random.randint(jax.random.fold_in(key, 21), (K, NB * DEVICES), 0, DEVICES)
    before = (owner + DEVICES - 1) % DEVICES
    across = (owner + DEVICES - DEVICES // 2) % DEVICES
    row_index = jnp.arange(K)[:, None]
    source = jnp.where(row_index == 0, before[None, :], source)
    source = jnp.where(row_index == 1, across[None, :], source)
    picked = jax.random.randint(jax.random.fold_in(key, 22), (K, NB * DEVICES), 0, CAP)
    live = counts[source, owner[None, :]]
    return (source * CAP + picked % jnp.maximum(live, 1)).astype(jnp.int32)


def draw_share_nodes(key, part):
    raw = jax.random.randint(jax.random.fold_in(key, 31), (DEVICES, DEVICES), 0, SH + 1)
    upper = jnp.triu(raw, 1)
    counts = upper + upper.T
    source = jnp.arange(DEVICES)[:, None]
    target = jnp.arange(DEVICES)[None, :]
    beside = (target == (source + 1) % DEVICES) | (source == (target + 1) % DEVICES)
    counts = jnp.where(beside & (source != target), SH, counts)
    counts = counts.at[0, 1].set(SH).at[1, 0].set(SH)
    counts = jnp.where(source == target, 0, counts)
    chosen = jax.random.randint(jax.random.fold_in(key, 32), (DEVICES, DEVICES, SH), 0, NODES_DEV)
    live = jnp.arange(SH)[None, None, :] < counts[:, :, None]
    return jnp.where(live, chosen, NODES_DEV).astype(jnp.int32)


def with_ends(values, rng, low, high):
    longest = values.shape.index(max(values.shape))
    spots = []
    for shift in (0, 1):
        where = [jax.random.randint(jax.random.fold_in(rng, axis), (), 0, length) for axis, length in enumerate(values.shape)]
        where[longest] = (where[longest] + shift) % values.shape[longest]
        spots.append(tuple(where))
    return values.at[spots[0]].set(low).at[spots[1]].set(high)


def levels(stream_key, extent, cuts, low, high):
    def one(dim, parts):
        steps = jax.random.uniform(jax.random.fold_in(jax.random.fold_in(stream_key, 6), dim), (parts,), jnp.float32, low / len(cuts), high / len(cuts))
        return jnp.repeat(jnp.exp(steps), extent[dim] // parts).reshape((-1,) + (1,) * (len(extent) - dim - 1))

    factor_of = one(*cuts[0])
    for cut in cuts[1:]:
        factor_of = factor_of * one(*cut)
    return factor_of


def gaussian(own_key, extent, spread, bound, cuts=(), held_as=jnp.bfloat16):
    result = spread * jax.random.normal(own_key, extent, jnp.float32)
    if cuts:
        result = result * levels(own_key, extent, cuts, -0.22, 0.18)
    return jnp.clip(result, -bound, bound).astype(held_as)


def setup_inputs(seed: int = 0) -> dict:
    streams_of = jax.random.split(jax.random.key(seed), 11)
    return {
        "fluid_state": gaussian(streams_of[0], (4, NX, NY, NZ), 0.5, 3.0, ((1, 8), (2, 16)), jnp.float32),
        "node_disp": gaussian(streams_of[1], (3, NODES), 0.005, 0.02, ((1, 128),), jnp.float32),
        "node_vel": gaussian(streams_of[2], (3, NODES), 0.3, 1.0, ((1, 128),), jnp.float32),
        "fiber_angles": jnp.clip(jax.random.uniform(streams_of[3], (2, ELEMS), jnp.float32, -3.140625, 3.140625), -3.140625, 3.140625),
        "connectivity": with_ends(jax.random.randint(streams_of[4], (27, ELEMS), 0, NODES_DEV), jax.random.fold_in(streams_of[4], 1), 0, NODES_DEV - 1).astype(jnp.int32),
        "send_blocks": draw_send_blocks(jax.random.fold_in(streams_of[10], 71), 0),
        "interp_slots": draw_interp_slots(jax.random.fold_in(streams_of[10], 71), 0),
        "weight_index": with_ends(jax.random.randint(streams_of[7], (K, NBLK), 0, WTAB), jax.random.fold_in(streams_of[7], 1), 0, WTAB - 1).astype(jnp.int32),
        "share_nodes": draw_share_nodes(jax.random.fold_in(streams_of[10], 71), 0),
        "weight_table": gaussian(streams_of[9], (WTAB, 128, 128), (K * 128) ** -0.5, 0.25),
    }


time_step = 0.1
viscosity = 1.0
sound_square = 1.0
penalty = 4.0
node_mass = 0.5
shear_modulus = 2.0
bulk_modulus = 4.0
fiber_stiff = 2.0
fiber_exponent = 1.0

def lagrange(degree, position):
    if degree == 0:
        return 0.5 * position * (position - 1.0)
    if degree == 1:
        return 1.0 - position * position
    return 0.5 * position * (position + 1.0)

def slope(degree, position):
    if degree == 0:
        return position - 0.5
    if degree == 1:
        return -2.0 * position
    return position + 0.5

def basis_function_array():
    points = (-1.0 / math.sqrt(3.0), 1.0 / math.sqrt(3.0))
    deriv_table = np.zeros((8, 3, 27))
    for quadrant in range(8):
        coords = (points[quadrant // 4], points[quadrant // 2 % 2], points[quadrant % 2])
        for corner in range(27):
            orders = (corner // 9, corner // 3 % 3, corner % 3)
            for direction in range(3):
                product_value = 2.0
                for factor_axis in range(3):
                    if factor_axis == direction:
                        product_value = product_value * slope(orders[factor_axis], coords[factor_axis])
                    else:
                        product_value = product_value * lagrange(orders[factor_axis], coords[factor_axis])
                deriv_table[quadrant, direction, corner] = product_value
    return jnp.asarray(deriv_table, dtype=jnp.float32)

def element_forces(displace, angles, connect, derivs):
    nodal_disp = displace[:, connect]
    strain = jnp.einsum('qja,iae->qije', derivs, nodal_disp, precision=lax.Precision.HIGHEST)
    identity_block = jnp.eye(3, dtype=jnp.float32)[None, :, :, None]
    deform = strain + identity_block
    leading_line = jnp.roll(deform, -1, axis=1)
    row_two = jnp.roll(deform, -2, axis=1)
    cofactor = jnp.roll(leading_line, -1, axis=2) * jnp.roll(row_two, -2, axis=2) - jnp.roll(leading_line, -2, axis=2) * jnp.roll(row_two, -1, axis=2)
    volume = lax.optimization_barrier(jnp.sum(deform[:, 0] * cofactor[:, 0], axis=1))
    fiber_dir = jnp.stack([jnp.cos(angles[0]) * jnp.cos(angles[1]), jnp.cos(angles[0]) * jnp.sin(angles[1]), jnp.sin(angles[0])])
    stretched = jnp.einsum('qije,je->qie', deform, fiber_dir, precision=lax.Precision.HIGHEST)
    excess = lax.optimization_barrier(jnp.sum(stretched * stretched, axis=1)) - 1.0
    fiber_weight = 2.0 * fiber_stiff * excess * jnp.exp(fiber_exponent * excess * excess)
    stress = shear_modulus * deform + (bulk_modulus * (volume - 1.0) - shear_modulus)[:, None, None, :] * cofactor
    stress = stress + fiber_weight[:, None, None, :] * stretched[:, :, None, :] * fiber_dir[None, None, :, :]
    elemental = -0.125 * jnp.einsum('qije,qja->iae', stress, derivs, precision=lax.Precision.HIGHEST)
    padded = jnp.zeros((3, displace.shape[1] + 1), jnp.float32)
    return padded.at[:, connect].add(elemental)

def neighbours(field):
    ahead = (field[:, 2:, 1:-1, 1:-1], field[:, 1:-1, 2:, 1:-1], field[:, 1:-1, 1:-1, 2:])
    behind = (field[:, :-2, 1:-1, 1:-1], field[:, 1:-1, :-2, 1:-1], field[:, 1:-1, 1:-1, :-2])
    return (ahead, behind)

def advance(padded, fluid_force):
    full = jnp.pad(padded, ((0, 0), (0, 0), (0, 0), (1, 1)))
    centre = full[:, 1:-1, 1:-1, 1:-1]
    motion = centre[:3]
    mass_per_volume = centre[3]
    flux = (1.0 + full[3:4]) * full[:3]
    flux_ahead, flux_behind = neighbours(flux)
    diverge = 0.5 * (flux_ahead[0][0] - flux_behind[0][0]) + 0.5 * (flux_ahead[1][1] - flux_behind[1][1]) + 0.5 * (flux_ahead[2][2] - flux_behind[2][2])
    move_ahead, move_behind = neighbours(full[:3])
    laplace = move_ahead[0] + move_behind[0] + move_ahead[1] + move_behind[1] + move_ahead[2] + move_behind[2] - 6.0 * motion
    dens_ahead, dens_behind = neighbours(full[3:4])
    gradient = jnp.concatenate([0.5 * (dens_ahead[0] - dens_behind[0]), 0.5 * (dens_ahead[1] - dens_behind[1]), 0.5 * (dens_ahead[2] - dens_behind[2])], axis=0)
    motion_new = motion + time_step * (viscosity * laplace - sound_square * gradient + fluid_force)
    density_new = mass_per_volume - time_step * diverge
    return jnp.concatenate([motion_new, density_new[None]], axis=0)

def to_blocks(field):
    tiles = field.reshape(3, N_GX, CX, N_GY, CY, NZ).transpose(0, 1, 3, 2, 4, 5)
    return tiles.reshape(3, N_GX * N_GY, FB, 128)

def from_blocks(blocks):
    tiles = blocks.reshape(3, N_GX, N_GY, CX, CY, NZ).transpose(0, 1, 3, 2, 4, 5)
    return tiles.reshape(3, NX, NY, NZ)

def reference(fluid_state, node_disp, node_vel, fiber_angles, connectivity, send_blocks, interp_slots, weight_index, share_nodes, weight_table):
    derivs = basis_function_array()
    part_count = N_GX * N_GY
    part_range = jnp.arange(part_count, dtype=jnp.int32)
    source_grid = jnp.broadcast_to(part_range[None, :, None], (part_count, part_count, SH))
    target_grid = jnp.broadcast_to(part_range[:, None, None], (part_count, part_count, SH))
    mirrored = jnp.transpose(share_nodes, (1, 0, 2))
    angle_parts = fiber_angles.reshape(2, part_count, ELEM_DEV).transpose(1, 0, 2)
    connect_parts = connectivity.reshape(27, part_count, ELEM_DEV).transpose(1, 0, 2)
    slot_parts = interp_slots.reshape(K, part_count, NB).transpose(1, 0, 2)
    windex_parts = weight_index.reshape(K, part_count, NB).transpose(1, 0, 2)
    displace = node_disp.reshape(3, part_count, NODES_DEV).transpose(1, 0, 2)
    velocity = node_vel.reshape(3, part_count, NODES_DEV).transpose(1, 0, 2)
    current = fluid_state
    for stepping in range(STEPS):
        rounded = lax.optimization_barrier(to_blocks(current[:3]).astype(jnp.bfloat16))
        blocks_pad = jnp.concatenate([rounded, jnp.zeros((3, part_count, 1, 128), jnp.bfloat16)], axis=2)
        elastic = lax.map(lambda packed: element_forces(packed[0], packed[1], packed[2], derivs), (displace, angle_parts, connect_parts))
        elastic = elastic.transpose(1, 0, 2)
        partner = elastic[:, source_grid, mirrored]
        summed = elastic.at[:, target_grid, share_nodes].add(partner)[:, :, :NODES_DEV]
        summed_parts = summed.transpose(1, 0, 2)

        def part_update(force_sum, packed):
            part_index, position_records, windex, total_force, part_disp, part_vel = packed
            source = part_range[:, None]
            column = lax.dynamic_index_in_dim(send_blocks, part_index, 1, keepdims=False)
            incoming_quantities = blocks_pad[:, source, column].reshape(3, part_count * CAP, 128).astype(jnp.float32)
            interpolated_quantities = jnp.zeros((3, NB, 128), jnp.float32)
            tile_entries = []
            for inclusion_indicator in range(K):
                patch_constituents = weight_table[windex[inclusion_indicator]].astype(jnp.float32)
                tile_entries.append(patch_constituents)
                interpolated_quantities = interpolated_quantities + jnp.einsum('kmn,mbn->kmb', incoming_quantities[:, position_records[inclusion_indicator]], patch_constituents, precision=lax.Precision.HIGHEST)
            coupling = penalty * (interpolated_quantities - part_vel.reshape(3, NB, 128))
            pushed_values = lax.optimization_barrier((-coupling).astype(jnp.bfloat16)).astype(jnp.float32)
            slot_forces_local = jnp.zeros((3, part_count * CAP, 128), jnp.float32)
            for inclusion_indicator in range(K):
                slot_forces_local = slot_forces_local.at[:, position_records[inclusion_indicator]].add(jnp.einsum('okj,kjx->okx', pushed_values, tile_entries[inclusion_indicator], precision=lax.Precision.HIGHEST))
            force_sum = force_sum.at[:, source, column].add(slot_forces_local.reshape(3, part_count, CAP, 128))
            new_vel = part_vel + time_step / node_mass * (total_force + coupling.reshape(3, NODES_DEV))
            new_disp = part_disp + time_step * new_vel
            return (force_sum, (new_disp, new_vel))
        force_init = jnp.zeros((3, part_count, FB + 1, 128), jnp.float32)
        force_sum, (displace, velocity) = lax.scan(part_update, force_init, (part_range, slot_parts, windex_parts, summed_parts, displace, velocity))
        fluid_force = from_blocks(force_sum[:, :, :FB])
        padded = jnp.pad(current, ((0, 0), (1, 1), (1, 1), (0, 0)))
        current = advance(padded, fluid_force)
    disp_out = displace.transpose(1, 0, 2).reshape(3, NODES)
    vel_out = velocity.transpose(1, 0, 2).reshape(3, NODES)
    return (current, disp_out, vel_out)
```

```python
import math

import jax
import jax.numpy as jnp
import numpy as np
from jax import lax
from jax.experimental import pallas as pl
from jax.experimental.pallas import tpu as pltpu
from jax.sharding import PartitionSpec as P

STEPS = 3

time_step = 0.1
viscosity = 1.0
sound_square = 1.0
penalty = 4.0
node_mass = 0.5
shear_modulus = 2.0
bulk_modulus = 4.0
fiber_stiff = 2.0
fiber_exponent = 1.0

BF16 = jnp.bfloat16
F32 = jnp.float32
AXES = ("gx", "gy")


def lagrange(degree, position):
    if degree == 0:
        return 0.5 * position * (position - 1.0)
    if degree == 1:
        return 1.0 - position * position
    return 0.5 * position * (position + 1.0)


def slope(degree, position):
    if degree == 0:
        return position - 0.5
    if degree == 1:
        return -2.0 * position
    return position + 0.5


def derivative_matrix():
    points = (-1.0 / math.sqrt(3.0), 1.0 / math.sqrt(3.0))
    table = np.zeros((8, 3, 27))
    for point in range(8):
        coords = (points[point // 4], points[point // 2 % 2], points[point % 2])
        for node in range(27):
            orders = (node // 9, node // 3 % 3, node % 3)
            for direction in range(3):
                value = 2.0
                for axis in range(3):
                    shape = slope if axis == direction else lagrange
                    value = value * shape(orders[axis], coords[axis])
                table[point, direction, node] = value
    table = table.astype(np.float32)
    big = np.zeros((72, 112), np.float32)
    for i in range(3):
        for j in range(3):
            for node in range(27):
                big[(3 * i + j) * 8 : (3 * i + j) * 8 + 8, node * 4 + i] = table[:, j, node]
    return big


def dot(a, b, precision=None):
    return lax.dot_general(
        a, b, (((1,), (0,)), ((), ())), precision=precision, preferred_element_type=F32
    )


def dot_nt(a, b):
    return lax.dot_general(a, b, (((1,), (1,)), ((), ())), preferred_element_type=F32)


def node_onehot(row):
    lane = row & 127
    return jnp.where(lax.broadcasted_iota(jnp.int32, (128, 512), 0) == lane, 1.0, 0.0).astype(BF16)


def node_high(row):
    return jnp.broadcast_to(row >> 7, (8, 512)) - (
        lax.broadcasted_iota(jnp.int32, (8, 512), 0) >> 2
    )


def pick_rows(table, high):
    picked = jnp.where(high == 0, table[0:8], 0.0)
    for r in range(1, 16):
        picked = picked + jnp.where(high == 2 * r, table[8 * r : 8 * r + 8], 0.0)
    return picked + pltpu.roll(picked, 4, 0)


def spread_rows(value, high):
    return jnp.concatenate([jnp.where(high == 2 * r, value, 0.0) for r in range(16)], axis=0)


def both_halves(value, odd):
    turned = pltpu.roll(value, 4, 0)
    low = lax.broadcasted_iota(jnp.int32, value.shape, 0) < 4
    return jnp.where(low, turned, value) if odd else jnp.where(low, value, turned)


def split(value):
    head = value.astype(BF16)
    return head, (value - head.astype(F32)).astype(BF16)


def elastic_kernel(
    disp_ref, idx_ref, fiber_ref, deriv_ref, derivt_ref, elastic_ref, shared_ref,
    nodal_ref, work_ref, turn_ref,
):
    head, tail = split(disp_ref[...])
    both = jnp.concatenate([head, tail], axis=1)

    def fetch(pair, carry):
        halves = []
        for s in range(2):
            row = idx_ref[pl.ds(2 * pair + s, 1), :]
            hot = node_onehot(row)
            table = dot(both, jnp.concatenate([hot, hot], axis=0))
            halves.append(pick_rows(table, node_high(row)))
        low = lax.broadcasted_iota(jnp.int32, (8, 512), 0) < 4
        nodal_ref[pl.ds(pl.multiple_of(8 * pair, 8), 8), :] = jnp.where(low, halves[0], halves[1])
        return carry

    lax.fori_loop(0, 14, fetch, 0)
    work_ref[...] = dot(deriv_ref[...], nodal_ref[...], lax.Precision.HIGHEST)

    def entry(i, j):
        value = work_ref[8 * (3 * i + j) : 8 * (3 * i + j) + 8, :]
        return value + 1.0 if i == j else value

    F = [[entry(i, j) for j in range(3)] for i in range(3)]
    fiber = [fiber_ref[j : j + 1, :] for j in range(3)]

    def cofactor(i, j):
        i1, i2, j1, j2 = (i + 1) % 3, (i + 2) % 3, (j + 1) % 3, (j + 2) % 3
        return F[i1][j1] * F[i2][j2] - F[i1][j2] * F[i2][j1]

    cof = [[cofactor(i, j) for j in range(3)] for i in range(3)]
    volume = F[0][0] * cof[0][0] + F[0][1] * cof[0][1] + F[0][2] * cof[0][2]
    along = [F[i][0] * fiber[0] + F[i][1] * fiber[1] + F[i][2] * fiber[2] for i in range(3)]
    excess = along[0] * along[0] + along[1] * along[1] + along[2] * along[2] - 1.0
    weight = 2.0 * fiber_stiff * excess * jnp.exp(fiber_exponent * excess * excess)
    factor = bulk_modulus * (volume - 1.0) - shear_modulus
    for i in range(3):
        pulled = weight * along[i]
        for j in range(3):
            work_ref[8 * (3 * i + j) : 8 * (3 * i + j) + 8, :] = (
                shear_modulus * F[i][j] + factor * cof[i][j] + pulled * fiber[j]
            )
    nodal_ref[...] = dot(derivt_ref[...], work_ref[...], lax.Precision.HIGHEST)

    def deposit(pair, total):
        rows = nodal_ref[pl.ds(pl.multiple_of(8 * pair, 8), 8), :]
        for s in range(2):
            row = idx_ref[pl.ds(2 * pair + s, 1), :]
            high = node_high(row)
            value = both_halves(rows, s == 1)
            value_head, value_tail = split(value)
            left = jnp.concatenate(
                [
                    spread_rows(value_head.astype(F32), high),
                    spread_rows(value_tail.astype(F32), high),
                ],
                axis=0,
            ).astype(BF16)
            both_parts = dot_nt(left, node_onehot(row))
            total = total + both_parts[:128] + both_parts[128:]
        return total

    elastic = lax.fori_loop(0, 14, deposit, jnp.zeros((128, 128), F32))
    elastic_ref[...] = elastic
    sent = elastic.astype(BF16)
    turn_ref[...] = jnp.zeros((128, 128), F32)
    for t in range(4):
        row = idx_ref[28 + t : 29 + t, :]
        picked = pick_rows(dot(sent, node_onehot(row)), node_high(row))
        for jj in range(4):
            turn_ref[16 * t + 4 * jj : 16 * t + 4 * jj + 4, :] = picked[0:4, 128 * jj : 128 * jj + 128]
    shared_ref[...] = turn_ref[...].T


def couple_kernel(
    windex_ref, recv_ref, vel_ref, pick_ref, pickt_ref, table_ref, shared_ref,
    payload_ref, coupling_ref, rows_ref, chosen_ref, spread_ref,
):
    rows_ref[...] = recv_ref[...].astype(F32)
    chosen_ref[...] = jnp.zeros((512, 128), F32)
    pick = pick_ref[...]
    for q in range(3):
        plane = rows_ref[pl.ds(q, 512, stride=4), :].astype(BF16)
        chosen_ref[pl.ds(q, 128, stride=4), :] = dot(pick, plane)

    def group(g, carry):
        start = pl.multiple_of(16 * g, 16)
        left = jnp.concatenate(
            [chosen_ref[pl.ds(128 * k + start, 16), :] for k in range(4)], axis=1
        ).astype(BF16)
        owner = lax.broadcasted_iota(jnp.int32, (16, 128), 0) >> 2
        weights = []
        sampled = jnp.zeros((16, 128), F32)
        for s in range(4):
            weight = jnp.concatenate(
                [table_ref[windex_ref[32 * k + 4 * g + s]] for k in range(4)], axis=1
            )
            weights.append(weight)
            sampled = jnp.where(owner == s, dot_nt(left, weight), sampled)
        coupling = penalty * (sampled - vel_ref[pl.ds(start, 16), :])
        coupling_ref[pl.ds(start, 16), :] = coupling
        pushed = (-coupling).astype(BF16)
        wide_owner = lax.broadcasted_iota(jnp.int32, (16, 512), 0) >> 2
        out = jnp.zeros((16, 512), F32)
        for s in range(4):
            out = jnp.where(wide_owner == s, dot(pushed, weights[s]), out)
        for k in range(4):
            spread_ref[pl.ds(128 * k + start, 16), :] = out[:, 128 * k : 128 * k + 128]
        return carry

    lax.fori_loop(0, 8, group, 0)
    pickt = pickt_ref[...]
    for q in range(3):
        head, tail = split(spread_ref[pl.ds(q, 128, stride=4), :])
        rows_ref[pl.ds(q, 512, stride=4), :] = dot(pickt, jnp.concatenate([head, tail], axis=0))
    rows_ref[pl.ds(3, 512, stride=4), :] = jnp.zeros((512, 128), F32)
    rows_ref[pl.ds(3, 128, stride=16), :] = shared_ref[...]
    payload_ref[...] = rows_ref[...].astype(BF16)


def write_payload(send, blocks_ref, rows_ref, payload_ref):
    sent = dot(send, blocks_ref[...])
    for q in range(3):
        rows_ref[pl.ds(q, 512, stride=4), :] = sent[:, 128 * q : 128 * q + 128]
    rows_ref[pl.ds(3, 512, stride=4), :] = jnp.zeros((512, 128), F32)
    payload_ref[...] = rows_ref[...].astype(BF16)


def store_blocks(blocks_ref, x, q, plane):
    for half in range(2):
        blocks_ref[128 * half + 16 * x : 128 * half + 16 * x + 16, 128 * q : 128 * q + 128] = plane[
            :, 128 * half : 128 * half + 128
        ].astype(BF16)


def pack_kernel(state_ref, send_ref, payload_ref, blocks_ref, rows_ref):
    for q in range(3):
        for x in range(8):
            store_blocks(blocks_ref, x, q, state_ref[q, x])
    write_payload(send_ref[...], blocks_ref, rows_ref, payload_ref)


def update_kernel(last):
    def kernel(
        recv_ref, state_ref, xlow_ref, xhigh_ref, ylow_ref, yhigh_ref, sendt_ref, send_ref,
        elastic_ref, coupling_ref, vel_ref, disp_ref, share_ref, *rest,
    ):
        if last:
            new_ref, velout_ref, dispout_ref, rows_ref, force_ref, turn_ref = rest
        else:
            (
                new_ref, velout_ref, dispout_ref, payload_ref, xlowout_ref, xhighout_ref,
                ylowout_ref, yhighout_ref, rows_ref, force_ref, turn_ref, blocks_ref,
            ) = rest
        rows_ref[...] = recv_ref[...].astype(F32)
        planes = jnp.concatenate(
            [rows_ref[pl.ds(q, 512, stride=4), :].astype(BF16) for q in range(3)], axis=1
        )
        force_ref[...] = dot(sendt_ref[...], planes)

        turn_ref[...] = rows_ref[pl.ds(3, 128, stride=16), :].T
        total = elastic_ref[...]
        for t in range(4):
            row = share_ref[t : t + 1, :]
            pieces = []
            for jj in range(4):
                first = 16 * t + 8 * (jj // 2)
                pieces.append(both_halves(turn_ref[first : first + 8, :], jj % 2 == 1))
            left = spread_rows(jnp.concatenate(pieces, axis=1), node_high(row)).astype(BF16)
            total = total + dot_nt(left, node_onehot(row))
        velocity = vel_ref[...] + time_step / node_mass * (total + coupling_ref[...])
        velout_ref[...] = velocity
        dispout_ref[...] = disp_ref[...] + time_step * velocity

        yrow = lax.broadcasted_iota(jnp.int32, (16, 256), 0)
        zlane = lax.broadcasted_iota(jnp.int32, (16, 256), 1)

        def around(f, x):
            centre = state_ref[f, x]
            xm = xlow_ref[f] if x == 0 else state_ref[f, x - 1]
            xp = xhigh_ref[f] if x == 7 else state_ref[f, x + 1]
            ym = jnp.where(yrow == 0, ylow_ref[f, x], pltpu.roll(centre, 1, 0))
            yp = jnp.where(yrow == 15, yhigh_ref[f, x], pltpu.roll(centre, 15, 0))
            zm = jnp.where(zlane == 0, 0.0, pltpu.roll(centre, 1, 1))
            zp = jnp.where(zlane == 255, 0.0, pltpu.roll(centre, 255, 1))
            return centre, ((xm, xp), (ym, yp), (zm, zp))

        for x in range(8):
            density, near = around(3, x)
            divergence = jnp.zeros((16, 256), F32)
            for q in range(3):
                centre, pairs = around(q, x)
                laplace = -6.0 * centre
                for below, above in pairs:
                    laplace = laplace + (below + above)
                gradient = 0.5 * (near[q][1] - near[q][0])
                below, above = pairs[q]
                divergence = divergence + 0.5 * (
                    (1.0 + near[q][1]) * above - (1.0 + near[q][0]) * below
                )
                force = jnp.concatenate(
                    [
                        force_ref[128 * h + 16 * x : 128 * h + 16 * x + 16, 128 * q : 128 * q + 128]
                        for h in range(2)
                    ],
                    axis=1,
                )
                fresh = centre + time_step * (
                    viscosity * laplace - sound_square * gradient + force
                )
                new_ref[q, x] = fresh
                if not last:
                    store_blocks(blocks_ref, x, q, fresh)
                    put_edges(q, x, fresh, xlowout_ref, xhighout_ref, ylowout_ref, yhighout_ref)
            fresh = density - time_step * divergence
            new_ref[3, x] = fresh
            if not last:
                put_edges(3, x, fresh, xlowout_ref, xhighout_ref, ylowout_ref, yhighout_ref)
        if not last:
            write_payload(send_ref[...], blocks_ref, rows_ref, payload_ref)

    return kernel


def put_edges(f, x, fresh, xlowout_ref, xhighout_ref, ylowout_ref, yhighout_ref):
    if x == 0:
        xlowout_ref[f] = fresh
    if x == 7:
        xhighout_ref[f] = fresh
    ylowout_ref[f, x] = fresh[0:1]
    yhighout_ref[f, x] = fresh[15:16]


VMEM = pl.BlockSpec(memory_space=pltpu.VMEM)
SMEM = pl.BlockSpec(memory_space=pltpu.SMEM)


def shape(dims, dtype=F32):
    return jax.ShapeDtypeStruct(dims, dtype)


def call(kernel, outs, specs, scratch, flops, name):
    return pl.pallas_call(
        kernel,
        out_shape=outs,
        in_specs=specs,
        out_specs=[VMEM] * len(outs),
        scratch_shapes=scratch,
        cost_estimate=pl.CostEstimate(flops=flops, transcendentals=0, bytes_accessed=2_000_000),
        compiler_params=pltpu.CompilerParams(vmem_limit_bytes=32 * 1024 * 1024),
        name=name,
    )


def exchange(payload):
    return lax.all_to_all(
        payload.reshape(128, 16, 128), AXES, split_axis=0, concat_axis=0, tiled=True
    ).reshape(2048, 128)


def halo(edges):
    xlow, xhigh, ylow, yhigh = edges

    def shift(low, high, axis):
        size = lax.axis_size(axis)
        up = [(i, i + 1) for i in range(size - 1)]
        down = [(b, a) for a, b in up]
        return lax.ppermute(high, axis, up), lax.ppermute(low, axis, down)

    xm, xp = shift(xlow, xhigh, "gx")
    ym, yp = shift(ylow, yhigh, "gy")
    return xm, xp, ym, yp


def to_rows(nodes):
    return jnp.pad(nodes.reshape(3, 32, 128).transpose(1, 0, 2), ((0, 0), (0, 1), (0, 0))).reshape(
        128, 128
    )


def from_rows(rows):
    return rows.reshape(32, 4, 128)[:, :3].transpose(1, 0, 2).reshape(3, 4096)


def body(
    fluid_state, node_disp, node_vel, fiber_angles, connectivity,
    send_blocks, interp_slots, weight_index, share_nodes, weight_table,
):
    big = derivative_matrix()
    deriv = jnp.asarray(big)
    derivt = jnp.asarray(-0.125 * big.T)
    unused = jnp.full((1, 512), 4096, jnp.int32)
    share = share_nodes[0].T.reshape(4, 512)
    index = jnp.concatenate([connectivity, unused, share], axis=0)
    fiber = jnp.stack(
        [
            jnp.cos(fiber_angles[0]) * jnp.cos(fiber_angles[1]),
            jnp.cos(fiber_angles[0]) * jnp.sin(fiber_angles[1]),
            jnp.sin(fiber_angles[0]),
        ]
    )
    sends = send_blocks[0].reshape(512)
    sends = jnp.where(sends < 256, (sends & 1) * 128 + (sends >> 1), -1)
    blocks_range = jnp.arange(256, dtype=jnp.int32)
    slots_range = jnp.arange(512, dtype=jnp.int32)
    send = (sends[:, None] == blocks_range[None, :]).astype(BF16)
    sendt = (blocks_range[:, None] == sends[None, :]).astype(BF16)
    slots = interp_slots.reshape(128)
    pick = (slots[:, None] == slots_range[None, :]).astype(BF16)
    twice = jnp.concatenate([slots, slots])
    pickt = (slots_range[:, None] == twice[None, :]).astype(BF16)
    windex = weight_index.reshape(128)

    elastic_call = call(
        elastic_kernel,
        [shape((128, 128)), shape((128, 128))],
        [VMEM] * 5,
        [pltpu.VMEM((112, 512), F32), pltpu.VMEM((72, 512), F32), pltpu.VMEM((128, 128), F32)],
        3_000_000_000,
        "elastic",
    )
    couple_call = call(
        couple_kernel,
        [shape((2048, 128), BF16), shape((128, 128))],
        [SMEM] + [VMEM] * 6,
        [
            pltpu.VMEM((2048, 128), F32),
            pltpu.VMEM((512, 128), F32),
            pltpu.VMEM((512, 128), F32),
        ],
        1_000_000_000,
        "couple",
    )
    pack_call = call(
        pack_kernel,
        [shape((2048, 128), BF16)],
        [VMEM] * 2,
        [pltpu.VMEM((256, 384), BF16), pltpu.VMEM((2048, 128), F32)],
        200_000_000,
        "pack",
    )

    def update_call(last):
        outs = [shape((4, 8, 16, 256)), shape((128, 128)), shape((128, 128))]
        scratch = [
            pltpu.VMEM((2048, 128), F32),
            pltpu.VMEM((256, 384), F32),
            pltpu.VMEM((128, 128), F32),
        ]
        if not last:
            outs = outs + [
                shape((2048, 128), BF16),
                shape((4, 16, 256)),
                shape((4, 16, 256)),
                shape((4, 8, 1, 256)),
                shape((4, 8, 1, 256)),
            ]
            scratch = scratch + [pltpu.VMEM((256, 384), BF16)]
        return call(
            update_kernel(last), outs, [VMEM] * 13, scratch, 500_000_000,
            "finish" if last else "update",
        )

    state = fluid_state
    displace = to_rows(node_disp)
    velocity = to_rows(node_vel)
    payload = pack_call(state, send)[0]
    edges = (state[:, 0], state[:, 7], state[:, :, 0:1], state[:, :, 15:16])
    for step in range(STEPS):
        last = step == STEPS - 1
        received = exchange(payload)
        around = halo(edges)
        elastic, shared = elastic_call(displace, index, fiber, deriv, derivt)
        outbound, coupling = couple_call(
            windex, received, velocity, pick, pickt, weight_table, shared
        )
        inbound = exchange(outbound)
        results = update_call(last)(
            inbound, state, *around, sendt, send, elastic, coupling, velocity, displace, share
        )
        state, velocity, displace = results[:3]
        if not last:
            payload = results[3]
            edges = results[4:8]
    return (state, from_rows(displace), from_rows(velocity))


def solution(mesh):
    placed = (
        P(None, "gx", "gy", None),
        P(None, AXES),
        P(None, AXES),
        P(None, AXES),
        P(None, AXES),
        P(AXES, None, None),
        P(None, AXES),
        P(None, AXES),
        P(AXES, None, None),
        P(),
    )
    return jax.shard_map(
        body,
        mesh=mesh,
        in_specs=placed,
        out_specs=(P(None, "gx", "gy", None), P(None, AXES), P(None, AXES)),
        check_vma=False,
    )
```

```python
import math

import jax
import jax.numpy as jnp
from jax import lax
from jax.experimental import pallas as pl
from jax.experimental.pallas import tpu as pltpu
from jax.sharding import PartitionSpec as P

STEPS = 3

time_step = 0.1
viscosity = 1.0
sound_square = 1.0
penalty = 4.0
node_mass = 0.5
shear_modulus = 2.0
bulk_modulus = 4.0
fiber_stiff = 2.0
fiber_exponent = 1.0

BF16 = jnp.bfloat16
F32 = jnp.float32
AXES = ("gx", "gy")
FETCH = 7
DEPOSIT = 7
GROUP = 2


def lagrange(degree, position):
    outer = 0.5 * position * position
    ends = jnp.where(degree == 0, outer - 0.5 * position, outer + 0.5 * position)
    return jnp.where(degree == 1, 1.0 - position * position, ends)


def slope(degree, position):
    ends = jnp.where(degree == 0, position - 0.5, position + 0.5)
    return jnp.where(degree == 1, -2.0 * position, ends)


def derivative_matrix(dims, row_axis):
    row = lax.broadcasted_iota(jnp.int32, dims, row_axis)
    column = lax.broadcasted_iota(jnp.int32, dims, 1 - row_axis)
    i = (row * 171) >> 12
    j = (row - 24 * i) >> 3
    point = row & 7
    node = column >> 2
    first = (node * 57) >> 9
    middle = (node * 43) >> 7
    orders = (first, middle - 3 * first, node - 3 * middle)
    coords = (point >> 2, (point >> 1) & 1, point & 1)
    value = jnp.where(((column & 3) == i) & (node < 27), 2.0, 0.0)
    for axis in range(3):
        position = jnp.where(coords[axis] == 0, -1.0 / math.sqrt(3.0), 1.0 / math.sqrt(3.0))
        value = value * jnp.where(
            j == axis, slope(orders[axis], position), lagrange(orders[axis], position)
        )
    return value


def dot(a, b, precision=None):
    return lax.dot_general(
        a, b, (((1,), (0,)), ((), ())), precision=precision, preferred_element_type=F32
    )


def dot_nt(a, b):
    return lax.dot_general(a, b, (((1,), (1,)), ((), ())), preferred_element_type=F32)


def node_onehot(row):
    lane = row & 127
    return jnp.where(lax.broadcasted_iota(jnp.int32, (128, 512), 0) == lane, 1.0, 0.0).astype(BF16)


def node_high(row):
    return jnp.broadcast_to(row >> 7, (8, 512)) - (
        lax.broadcasted_iota(jnp.int32, (8, 512), 0) >> 2
    )


def pick_rows(table, high):
    picked = jnp.where(high == 0, table[0:8], 0.0)
    for r in range(1, 16):
        picked = picked + jnp.where(high == 2 * r, table[8 * r : 8 * r + 8], 0.0)
    return picked + pltpu.roll(picked, 4, 0)


def spread_rows(value, high):
    return jnp.concatenate([jnp.where(high == 2 * r, value, 0.0) for r in range(16)], axis=0)


def both_halves(value, odd):
    turned = pltpu.roll(value, 4, 0)
    low = lax.broadcasted_iota(jnp.int32, value.shape, 0) < 4
    return jnp.where(low, turned, value) if odd else jnp.where(low, value, turned)


def split(value):
    head = value.astype(BF16)
    return head, (value - head.astype(F32)).astype(BF16)


def elastic_kernel(first):
    def kernel(*refs):
        if first:
            (
                elastic_ref, shared_ref, rows_ref, velrows_ref, deriv_ref, derivt_ref, fiber_ref,
            ) = refs[5:12]
            nodal_ref, work_ref, turn_ref = refs[12:15]
            loaded, sems = refs[15:20], refs[20]
            loads = [pltpu.make_async_copy(refs[n], loaded[n], sems.at[n]) for n in range(5)]
            for load in loads:
                load.start()
            disp_ref, vel_ref, conn_ref, share_ref, angle_ref = loaded
            for load in loads:
                load.wait()
            rows_ref[...] = jnp.zeros((128, 128), F32)
            velrows_ref[...] = jnp.zeros((128, 128), F32)
            for h in range(32):
                rows_ref[4 * h : 4 * h + 3, :] = disp_ref[h]
                velrows_ref[4 * h : 4 * h + 3, :] = vel_ref[h]
            deriv_ref[...] = derivative_matrix((72, 112), 0)
            derivt_ref[...] = -0.125 * derivative_matrix((112, 72), 1)
            angles = angle_ref[...]
            cosine, sine = jnp.cos(angles), jnp.sin(angles)
            fiber_ref[0:1, :] = cosine[0:1] * cosine[1:2]
            fiber_ref[1:2, :] = cosine[0:1] * sine[1:2]
            fiber_ref[2:3, :] = sine[0:1]
        else:
            rows_ref, conn_ref, share_ref, deriv_ref, derivt_ref, fiber_ref = refs[:6]
            elastic_ref, shared_ref, nodal_ref, work_ref, turn_ref = refs[6:]
        elastic_forces(
            rows_ref, conn_ref, deriv_ref, derivt_ref, fiber_ref, elastic_ref, nodal_ref, work_ref
        )
        share_forces(elastic_ref, share_ref, shared_ref, turn_ref)

    return kernel


def elastic_forces(
    disp_ref, conn_ref, deriv_ref, derivt_ref, fiber_ref, elastic_ref, nodal_ref, work_ref
):
    head, tail = split(disp_ref[...])
    both = jnp.concatenate([head, tail], axis=1)

    def connect(node):
        return conn_ref[pl.ds(jnp.minimum(node, 26), 1), :]

    def fetch(turn, carry):
        for pair in [turn * FETCH + u for u in range(FETCH)]:
            halves = []
            for s in range(2):
                row = connect(2 * pair + s)
                hot = node_onehot(row)
                table = dot(both, jnp.concatenate([hot, hot], axis=0))
                halves.append(pick_rows(table, node_high(row)))
            low = lax.broadcasted_iota(jnp.int32, (8, 512), 0) < 4
            nodal_ref[pl.ds(pl.multiple_of(8 * pair, 8), 8), :] = jnp.where(
                low, halves[0], halves[1]
            )
        return carry

    lax.fori_loop(0, 14 // FETCH, fetch, 0)
    work_ref[...] = dot(deriv_ref[...], nodal_ref[...], lax.Precision.HIGHEST)

    def entry(i, j):
        value = work_ref[8 * (3 * i + j) : 8 * (3 * i + j) + 8, :]
        return value + 1.0 if i == j else value

    F = [[entry(i, j) for j in range(3)] for i in range(3)]
    fiber = [fiber_ref[j : j + 1, :] for j in range(3)]

    def cofactor(i, j):
        i1, i2, j1, j2 = (i + 1) % 3, (i + 2) % 3, (j + 1) % 3, (j + 2) % 3
        return F[i1][j1] * F[i2][j2] - F[i1][j2] * F[i2][j1]

    cof = [[cofactor(i, j) for j in range(3)] for i in range(3)]
    volume = F[0][0] * cof[0][0] + F[0][1] * cof[0][1] + F[0][2] * cof[0][2]
    along = [F[i][0] * fiber[0] + F[i][1] * fiber[1] + F[i][2] * fiber[2] for i in range(3)]
    excess = along[0] * along[0] + along[1] * along[1] + along[2] * along[2] - 1.0
    weight = 2.0 * fiber_stiff * excess * jnp.exp(fiber_exponent * excess * excess)
    factor = bulk_modulus * (volume - 1.0) - shear_modulus
    for i in range(3):
        pulled = weight * along[i]
        for j in range(3):
            work_ref[8 * (3 * i + j) : 8 * (3 * i + j) + 8, :] = (
                shear_modulus * F[i][j] + factor * cof[i][j] + pulled * fiber[j]
            )
    nodal_ref[...] = dot(derivt_ref[...], work_ref[...], lax.Precision.HIGHEST)

    def deposit(turn, total):
        for pair in [turn * DEPOSIT + u for u in range(DEPOSIT)]:
            rows = nodal_ref[pl.ds(pl.multiple_of(8 * pair, 8), 8), :]
            for s in range(2):
                row = connect(2 * pair + s)
                high = node_high(row)
                value_head, value_tail = split(both_halves(rows, s == 1))
                left = jnp.concatenate(
                    [
                        spread_rows(value_head.astype(F32), high),
                        spread_rows(value_tail.astype(F32), high),
                    ],
                    axis=0,
                ).astype(BF16)
                both_parts = dot_nt(left, node_onehot(row))
                total = total + both_parts[:128] + both_parts[128:]
        return total

    elastic_ref[...] = lax.fori_loop(0, 14 // DEPOSIT, deposit, jnp.zeros((128, 128), F32))


def share_row(share_ref, t):
    return jnp.concatenate([share_ref[4 * t + u : 4 * t + u + 1, :] for u in range(4)], axis=1)


def share_forces(elastic_ref, share_ref, shared_ref, turn_ref):
    sent = elastic_ref[...].astype(BF16)
    turn_ref[...] = jnp.zeros((128, 128), F32)
    for t in range(4):
        row = share_row(share_ref, t)
        picked = pick_rows(dot(sent, node_onehot(row)), node_high(row))
        for jj in range(4):
            turn_ref[16 * t + 4 * jj : 16 * t + 4 * jj + 4, :] = picked[0:4, 128 * jj : 128 * jj + 128]
    shared_ref[...] = turn_ref[...].T


def take_plane(rows_ref, q, stride):
    pieces = [rows_ref[pl.ds(3 * j + q, 128, stride=stride), :] for j in range(4)]
    return jnp.concatenate(pieces, axis=0).astype(BF16)


def put_plane(rows_ref, q, stride, plane):
    for j in range(4):
        rows_ref[pl.ds(3 * j + q, 128, stride=stride), :] = plane[128 * j : 128 * j + 128]


def couple_kernel(
    windex_ref, recv_ref, vel_ref, pick_ref, pickt_ref, table_ref, shared_ref,
    payload_ref, coupling_ref, rows_ref, chosen_ref, spread_ref, buffer_ref, sems,
):
    for g in range(8):
        for s in range(4):
            for k in range(4):
                pltpu.make_async_copy(
                    table_ref.at[windex_ref[k, 4 * g + s]],
                    buffer_ref.at[16 * g + 4 * s + k],
                    sems.at[g],
                ).start()
    rows_ref[0:1536, :] = recv_ref[...].astype(F32)
    chosen_ref[...] = jnp.zeros((512, 128), F32)
    pick = pick_ref[...]
    for q in range(3):
        chosen_ref[pl.ds(q, 128, stride=4), :] = dot(pick, take_plane(rows_ref, q, 12))

    def group(g, carry):
        part = pl.ds(pl.multiple_of(16 * g, 16), 16)
        pltpu.make_async_copy(table_ref.at[pl.ds(0, 16)], buffer_ref.at[part], sems.at[g]).wait()
        start = pl.multiple_of(16 * g, 16)
        left = jnp.concatenate(
            [chosen_ref[pl.ds(128 * k + start, 16), :] for k in range(4)], axis=1
        ).astype(BF16)
        owner = lax.broadcasted_iota(jnp.int32, (16, 128), 0) >> 2
        weights = []
        sampled = jnp.zeros((16, 128), F32)
        for s in range(4):
            weight = jnp.concatenate(
                [buffer_ref[16 * g + 4 * s + k] for k in range(4)], axis=1
            )
            weights.append(weight)
            sampled = jnp.where(owner == s, dot_nt(left, weight), sampled)
        coupling = penalty * (sampled - vel_ref[pl.ds(start, 16), :])
        coupling_ref[pl.ds(start, 16), :] = coupling
        pushed = (-coupling).astype(BF16)
        wide_owner = lax.broadcasted_iota(jnp.int32, (16, 512), 0) >> 2
        out = jnp.zeros((16, 512), F32)
        for s in range(4):
            out = jnp.where(wide_owner == s, dot(pushed, weights[s]), out)
        for k in range(4):
            spread_ref[pl.ds(128 * k + start, 16), :] = out[:, 128 * k : 128 * k + 128]
        return carry

    def groups(turn, carry):
        for u in range(GROUP):
            group(turn * GROUP + u, carry)
        return carry

    lax.fori_loop(0, 8 // GROUP, groups, 0)
    pickt = pickt_ref[...]
    for q in range(3):
        head, tail = split(spread_ref[pl.ds(q, 128, stride=4), :])
        put_plane(rows_ref, q, 14, dot(pickt, jnp.concatenate([head, tail], axis=0)))
    rows_ref[pl.ds(12, 128, stride=14), :] = shared_ref[...]
    rows_ref[pl.ds(13, 128, stride=14), :] = jnp.zeros((128, 128), F32)
    payload_ref[...] = rows_ref[...].astype(BF16)


def write_payload(send, blocks_ref, rows_ref, payload_ref):
    sent = dot(send, blocks_ref[...])
    for q in range(3):
        put_plane(rows_ref, q, 12, sent[:, 128 * q : 128 * q + 128])
    payload_ref[...] = rows_ref[0:1536, :].astype(BF16)


def store_blocks(blocks_ref, x, q, plane):
    for half in range(2):
        blocks_ref[128 * half + 16 * x : 128 * half + 16 * x + 16, 128 * q : 128 * q + 128] = plane[
            :, 128 * half : 128 * half + 128
        ].astype(BF16)


def pack_kernel(state_ref, send_ref, payload_ref, blocks_ref, rows_ref):
    for q in range(3):
        for x in range(8):
            store_blocks(blocks_ref, x, q, state_ref[q, x])
    write_payload(send_ref[...], blocks_ref, rows_ref, payload_ref)


def update_kernel(last):
    def kernel(
        recv_ref, state_ref, xlow_ref, xhigh_ref, ylow_ref, yhigh_ref, sendt_ref, send_ref,
        elastic_ref, coupling_ref, vel_ref, disp_ref, share_ref, *rest,
    ):
        if last:
            new_ref, velout_ref, dispout_ref, rows_ref, force_ref, turn_ref = rest
        else:
            (
                new_ref, velout_ref, dispout_ref, payload_ref, xlowout_ref, xhighout_ref,
                ylowout_ref, yhighout_ref, rows_ref, force_ref, turn_ref, blocks_ref,
            ) = rest
        rows_ref[...] = recv_ref[...].astype(F32)
        planes = jnp.concatenate(
            [take_plane(rows_ref, q, 14) for q in range(3)], axis=1
        )
        force_ref[...] = dot(sendt_ref[...], planes)

        turn_ref[...] = rows_ref[pl.ds(12, 128, stride=14), :].T
        total = elastic_ref[...]
        for t in range(4):
            row = share_row(share_ref, t)
            pieces = []
            for jj in range(4):
                first = 16 * t + 8 * (jj // 2)
                pieces.append(both_halves(turn_ref[first : first + 8, :], jj % 2 == 1))
            left = spread_rows(jnp.concatenate(pieces, axis=1), node_high(row)).astype(BF16)
            total = total + dot_nt(left, node_onehot(row))
        velocity = vel_ref[...] + time_step / node_mass * (total + coupling_ref[...])
        displace = disp_ref[...] + time_step * velocity
        if last:
            for h in range(32):
                velout_ref[h] = velocity[4 * h : 4 * h + 3]
                dispout_ref[h] = displace[4 * h : 4 * h + 3]
        else:
            velout_ref[...] = velocity
            dispout_ref[...] = displace

        yrow = lax.broadcasted_iota(jnp.int32, (16, 256), 0)
        zlane = lax.broadcasted_iota(jnp.int32, (16, 256), 1)

        def around(f, x):
            centre = state_ref[f, x]
            xm = xlow_ref[f] if x == 0 else state_ref[f, x - 1]
            xp = xhigh_ref[f] if x == 7 else state_ref[f, x + 1]
            ym = jnp.where(yrow == 0, ylow_ref[f, x], pltpu.roll(centre, 1, 0))
            yp = jnp.where(yrow == 15, yhigh_ref[f, x], pltpu.roll(centre, 15, 0))
            zm = jnp.where(zlane == 0, 0.0, pltpu.roll(centre, 1, 1))
            zp = jnp.where(zlane == 255, 0.0, pltpu.roll(centre, 255, 1))
            return centre, ((xm, xp), (ym, yp), (zm, zp))

        for x in range(8):
            density, near = around(3, x)
            divergence = jnp.zeros((16, 256), F32)
            for q in range(3):
                centre, pairs = around(q, x)
                laplace = -6.0 * centre
                for below, above in pairs:
                    laplace = laplace + (below + above)
                gradient = 0.5 * (near[q][1] - near[q][0])
                below, above = pairs[q]
                divergence = divergence + 0.5 * (
                    (1.0 + near[q][1]) * above - (1.0 + near[q][0]) * below
                )
                force = jnp.concatenate(
                    [
                        force_ref[128 * h + 16 * x : 128 * h + 16 * x + 16, 128 * q : 128 * q + 128]
                        for h in range(2)
                    ],
                    axis=1,
                )
                fresh = centre + time_step * (
                    viscosity * laplace - sound_square * gradient + force
                )
                new_ref[q, x] = fresh
                if not last:
                    store_blocks(blocks_ref, x, q, fresh)
                    put_edges(q, x, fresh, xlowout_ref, xhighout_ref, ylowout_ref, yhighout_ref)
            fresh = density - time_step * divergence
            new_ref[3, x] = fresh
            if not last:
                put_edges(3, x, fresh, xlowout_ref, xhighout_ref, ylowout_ref, yhighout_ref)
        if not last:
            write_payload(send_ref[...], blocks_ref, rows_ref, payload_ref)

    return kernel


def put_edges(f, x, fresh, xlowout_ref, xhighout_ref, ylowout_ref, yhighout_ref):
    if x == 0:
        xlowout_ref[f] = fresh
    if x == 7:
        xhighout_ref[f] = fresh
    ylowout_ref[f, x] = fresh[0:1]
    yhighout_ref[f, x] = fresh[15:16]


VMEM = pl.BlockSpec(memory_space=pltpu.VMEM)
SMEM = pl.BlockSpec(memory_space=pltpu.SMEM)
HBM = pl.BlockSpec(memory_space=pltpu.HBM)


def far(array):
    return pltpu.with_memory_space_constraint(array, pltpu.HBM)


def shape(dims, dtype=F32):
    return jax.ShapeDtypeStruct(dims, dtype)


def call(kernel, outs, specs, scratch, flops, name, mebibytes, out_specs=None):
    return pl.pallas_call(
        kernel,
        out_shape=outs,
        in_specs=specs,
        out_specs=out_specs or [VMEM] * len(outs),
        scratch_shapes=scratch,
        cost_estimate=pl.CostEstimate(flops=flops, transcendentals=0, bytes_accessed=2_000_000),
        compiler_params=pltpu.CompilerParams(vmem_limit_bytes=mebibytes * 1024 * 1024),
        name=name,
    )


def elastic_call(first):
    outs = [shape((128, 128))] * 2
    out_specs = [VMEM] * 2
    specs = [VMEM] * 6
    scratch = [
        pltpu.VMEM((112, 512), F32), pltpu.VMEM((72, 512), F32), pltpu.VMEM((128, 128), F32)
    ]
    if first:
        specs = [HBM] * 5
        scratch = scratch + [
            pltpu.VMEM((32, 3, 128), F32),
            pltpu.VMEM((32, 3, 128), F32),
            pltpu.VMEM((27, 512), jnp.int32),
            pltpu.VMEM((16, 128), jnp.int32),
            pltpu.VMEM((2, 512), F32),
            pltpu.SemaphoreType.DMA((5,)),
        ]
        out_specs = out_specs + [VMEM] * 5
        outs = outs + [shape((128, 128))] * 2
        outs = outs + [shape((72, 112)), shape((112, 72)), shape((3, 512))]
    return call(
        elastic_kernel(first),
        outs,
        specs,
        scratch,
        3_000_000_000,
        "elastic_first" if first else "elastic",
        16,
        out_specs,
    )


def couple_call():
    return call(
        couple_kernel,
        [shape((1792, 128), BF16), shape((128, 128))],
        [SMEM] + [VMEM] * 4 + [HBM, VMEM],
        [
            pltpu.VMEM((1792, 128), F32),
            pltpu.VMEM((512, 128), F32),
            pltpu.VMEM((512, 128), F32),
            pltpu.VMEM((128, 128, 128), BF16),
            pltpu.SemaphoreType.DMA((8,)),
        ],
        1_000_000_000,
        "couple",
        24,
    )


def pack_call():
    return call(
        pack_kernel,
        [shape((1536, 128), BF16)],
        [VMEM] * 2,
        [pltpu.VMEM((256, 384), BF16), pltpu.VMEM((1792, 128), F32)],
        200_000_000,
        "pack",
        16,
    )


def update_call(last):
    nodes = shape((32, 3, 128)) if last else shape((128, 128))
    outs = [shape((4, 8, 16, 256)), nodes, nodes]
    scratch = [
        pltpu.VMEM((1792, 128), F32),
        pltpu.VMEM((256, 384), F32),
        pltpu.VMEM((128, 128), F32),
    ]
    if not last:
        outs = outs + [
            shape((1536, 128), BF16),
            shape((4, 16, 256)),
            shape((4, 16, 256)),
            shape((4, 8, 1, 256)),
            shape((4, 8, 1, 256)),
        ]
        scratch = scratch + [pltpu.VMEM((256, 384), BF16)]
    return call(
        update_kernel(last), outs, [VMEM] * 13, scratch, 500_000_000,
        "finish" if last else "update", 16,
    )


def exchange(payload, dims):
    moved = lax.all_to_all(
        payload.reshape((128,) + dims + (128,)), AXES, split_axis=0, concat_axis=0, tiled=True
    )
    return moved.reshape(-1, 128)


def halo(edges):
    xlow, xhigh, ylow, yhigh = edges

    def shift(low, high, axis):
        size = lax.axis_size(axis)
        up = [(i, i + 1) for i in range(size - 1)]
        down = [(b, a) for a, b in up]
        return lax.ppermute(high, axis, up), lax.ppermute(low, axis, down)

    xm, xp = shift(xlow, xhigh, "gx")
    ym, yp = shift(ylow, yhigh, "gy")
    return xm, xp, ym, yp


def body(
    fluid_state, node_disp, node_vel, fiber_angles, connectivity,
    send_blocks, interp_slots, weight_index, share_nodes, weight_table,
):
    share = share_nodes[0].T
    sends = send_blocks[0].T
    sends = jnp.where(sends < 256, (sends & 1) * 128 + (sends >> 1), -1)
    blocks_range = jnp.arange(256, dtype=jnp.int32)
    slots_range = jnp.arange(512, dtype=jnp.int32)
    send = (sends[:, :, None] == blocks_range[None, None, :]).astype(BF16).reshape(512, 256)
    sendt = (blocks_range[:, None] == sends.reshape(512)[None, :]).astype(BF16)
    slots = (interp_slots & 3) * 128 + (interp_slots >> 2)
    pick = (slots[:, :, None] == slots_range[None, None, :]).astype(BF16).reshape(128, 512)
    flat = slots.reshape(128)
    pickt = (slots_range[:, None] == jnp.concatenate([flat, flat])[None, :]).astype(BF16)

    state = fluid_state
    payload = pack_call()(state, send)[0]
    edges = (state[:, 0], state[:, 7], state[:, :, 0:1], state[:, :, 15:16])
    for step in range(STEPS):
        last = step == STEPS - 1
        received = exchange(payload, (3, 4))
        around = halo(edges)
        if step == 0:
            start_disp = node_disp.reshape(3, 32, 128).transpose(1, 0, 2)
            start_vel = node_vel.reshape(3, 32, 128).transpose(1, 0, 2)
            elastic, shared, displace, velocity, *tables = elastic_call(True)(
                *map(far, (start_disp, start_vel, connectivity, share, fiber_angles))
            )
        else:
            elastic, shared = elastic_call(False)(displace, connectivity, share, *tables)
        outbound, coupling = couple_call()(
            far(weight_index), received, velocity, pick, pickt, far(weight_table), shared
        )
        inbound = exchange(outbound, (7, 2))
        results = update_call(last)(
            inbound, state, *around, sendt, send, elastic, coupling, velocity, displace, share
        )
        state, velocity, displace = results[:3]
        if not last:
            payload = results[3]
            edges = results[4:8]
    out = [nodes.transpose(1, 0, 2).reshape(3, 4096) for nodes in (displace, velocity)]
    return (state, out[0], out[1])


def solution(mesh):
    placed = (
        P(None, "gx", "gy", None),
        P(None, AXES),
        P(None, AXES),
        P(None, AXES),
        P(None, AXES),
        P(AXES, None, None),
        P(None, AXES),
        P(None, AXES),
        P(AXES, None, None),
        P(),
    )
    return jax.shard_map(
        body,
        mesh=mesh,
        in_specs=placed,
        out_specs=(P(None, "gx", "gy", None), P(None, AXES), P(None, AXES)),
        check_vma=False,
    )
```

```python
import math

import jax
import jax.numpy as jnp
from jax import lax
from jax.experimental import pallas as pl
from jax.experimental.pallas import tpu as pltpu
from jax.sharding import PartitionSpec as P


STEPS = 3

time_step = 0.1
viscosity = 1.0
sound_square = 1.0
penalty = 4.0
node_mass = 0.5
shear_modulus = 2.0
bulk_modulus = 4.0
fiber_stiff = 2.0
fiber_exponent = 1.0

BF16 = jnp.bfloat16
F32 = jnp.float32
AXES = ("gx", "gy")
FETCH = 7
DEPOSIT = 7
GROUP = 8


def lagrange(degree, position):
    outer = 0.5 * position * position
    ends = jnp.where(degree == 0, outer - 0.5 * position, outer + 0.5 * position)
    return jnp.where(degree == 1, 1.0 - position * position, ends)


def slope(degree, position):
    ends = jnp.where(degree == 0, position - 0.5, position + 0.5)
    return jnp.where(degree == 1, -2.0 * position, ends)


def derivative_matrix(dims, row_axis):
    row = lax.broadcasted_iota(jnp.int32, dims, row_axis)
    column = lax.broadcasted_iota(jnp.int32, dims, 1 - row_axis)
    i = (row * 171) >> 12
    j = (row - 24 * i) >> 3
    point = row & 7
    node = column >> 2
    first = (node * 57) >> 9
    middle = (node * 43) >> 7
    orders = (first, middle - 3 * first, node - 3 * middle)
    coords = (point >> 2, (point >> 1) & 1, point & 1)
    value = jnp.where(((column & 3) == i) & (node < 27), 2.0, 0.0)
    for axis in range(3):
        position = jnp.where(coords[axis] == 0, -1.0 / math.sqrt(3.0), 1.0 / math.sqrt(3.0))
        value = value * jnp.where(
            j == axis, slope(orders[axis], position), lagrange(orders[axis], position)
        )
    return value


def dot(a, b, precision=None):
    return lax.dot_general(
        a, b, (((1,), (0,)), ((), ())), precision=precision, preferred_element_type=F32
    )


def dot_nt(a, b):
    return lax.dot_general(a, b, (((1,), (1,)), ((), ())), preferred_element_type=F32)


def packed_offset(values, shift):
    rows = lax.broadcasted_iota(jnp.int32, (16, 512), 0) >> shift
    return (jnp.broadcast_to(values, (16, 512)) - rows).astype(F32).astype(BF16)


def node_onehot(row):
    offset = packed_offset(row & 127, 0)
    one, zero = jnp.ones((16, 512), BF16), jnp.zeros((16, 512), BF16)
    return jnp.concatenate(
        [jnp.where(offset == jnp.asarray(16 * r, BF16), one, zero) for r in range(8)], axis=0
    )


def pick_rows(table, row):
    high = jnp.broadcast_to(row >> 7, (8, 512)) - (
        lax.broadcasted_iota(jnp.int32, (8, 512), 0) >> 2
    )
    picked = jnp.where(high == 0, table[0:8], 0.0)
    for r in range(1, 16):
        picked = jnp.where(high == 2 * r, table[8 * r : 8 * r + 8], picked)
    return picked + pltpu.roll(picked, 4, 0)


def spread_rows(value, row):
    high = packed_offset(row >> 7, 2)
    wide = jnp.concatenate([value, value], axis=0).astype(BF16)
    zero = jnp.zeros((16, 512), BF16)
    return jnp.concatenate(
        [jnp.where(high == jnp.asarray(4 * r, BF16), wide, zero) for r in range(8)], axis=0
    )


def both_halves(value, odd):
    turned = pltpu.roll(value, 4, 0)
    low = lax.broadcasted_iota(jnp.int32, value.shape, 0) < 4
    return jnp.where(low, turned, value) if odd else jnp.where(low, value, turned)


def split(value):
    head = value.astype(BF16)
    return head, (value - head.astype(F32)).astype(BF16)


def elastic_kernel(first):
    def kernel(*refs):
        if first:
            (
                elastic_ref, shared_ref, rows_ref, velrows_ref, deriv_ref, derivt_ref, fiber_ref,
            ) = refs[5:12]
            nodal_ref, work_ref, turn_ref = refs[12:15]
            loaded, sems = refs[15:20], refs[20]
            loads = [pltpu.make_async_copy(refs[n], loaded[n], sems.at[n]) for n in range(5)]
            for load in loads:
                load.start()
            disp_ref, vel_ref, conn_ref, share_ref, angle_ref = loaded
            for load in loads:
                load.wait()
            rows_ref[...] = jnp.zeros((128, 128), F32)
            velrows_ref[...] = jnp.zeros((128, 128), F32)
            for h in range(32):
                rows_ref[4 * h : 4 * h + 3, :] = disp_ref[h]
                velrows_ref[4 * h : 4 * h + 3, :] = vel_ref[h]
            deriv_ref[...] = derivative_matrix((72, 112), 0)
            derivt_ref[...] = -0.125 * derivative_matrix((112, 72), 1)
            angles = angle_ref[...]
            cosine, sine = jnp.cos(angles), jnp.sin(angles)
            fiber_ref[0:1, :] = cosine[0:1] * cosine[1:2]
            fiber_ref[1:2, :] = cosine[0:1] * sine[1:2]
            fiber_ref[2:3, :] = sine[0:1]
        else:
            rows_ref, conn_ref, share_ref, deriv_ref, derivt_ref, fiber_ref = refs[:6]
            elastic_ref, shared_ref, nodal_ref, work_ref, turn_ref = refs[6:]
        elastic_forces(
            rows_ref, conn_ref, deriv_ref, derivt_ref, fiber_ref, elastic_ref, nodal_ref, work_ref
        )
        share_forces(elastic_ref, share_ref, shared_ref, turn_ref)

    return kernel


def elastic_forces(
    disp_ref, conn_ref, deriv_ref, derivt_ref, fiber_ref, elastic_ref, nodal_ref, work_ref
):
    head, tail = split(disp_ref[...])
    both = jnp.concatenate([head, tail], axis=1)

    def connect(node):
        return conn_ref[pl.ds(jnp.minimum(node, 26), 1), :]

    def fetch(turn, carry):
        for pair in [turn * FETCH + u for u in range(FETCH)]:
            halves = []
            for s in range(2):
                row = connect(2 * pair + s)
                hot = node_onehot(row)
                table = dot(both, jnp.concatenate([hot, hot], axis=0))
                halves.append(pick_rows(table, row))
            low = lax.broadcasted_iota(jnp.int32, (8, 512), 0) < 4
            nodal_ref[pl.ds(pl.multiple_of(8 * pair, 8), 8), :] = jnp.where(
                low, halves[0], halves[1]
            )
        return carry

    lax.fori_loop(0, 14 // FETCH, fetch, 0)
    work_ref[...] = dot(deriv_ref[...], nodal_ref[...], lax.Precision.HIGHEST)

    def entry(i, j):
        value = work_ref[8 * (3 * i + j) : 8 * (3 * i + j) + 8, :]
        return value + 1.0 if i == j else value

    F = [[entry(i, j) for j in range(3)] for i in range(3)]
    fiber = [fiber_ref[j : j + 1, :] for j in range(3)]

    def cofactor(i, j):
        i1, i2, j1, j2 = (i + 1) % 3, (i + 2) % 3, (j + 1) % 3, (j + 2) % 3
        return F[i1][j1] * F[i2][j2] - F[i1][j2] * F[i2][j1]

    cof = [[cofactor(i, j) for j in range(3)] for i in range(3)]
    volume = F[0][0] * cof[0][0] + F[0][1] * cof[0][1] + F[0][2] * cof[0][2]
    along = [F[i][0] * fiber[0] + F[i][1] * fiber[1] + F[i][2] * fiber[2] for i in range(3)]
    excess = along[0] * along[0] + along[1] * along[1] + along[2] * along[2] - 1.0
    weight = 2.0 * fiber_stiff * excess * jnp.exp(fiber_exponent * excess * excess)
    factor = bulk_modulus * (volume - 1.0) - shear_modulus
    for i in range(3):
        pulled = weight * along[i]
        for j in range(3):
            work_ref[8 * (3 * i + j) : 8 * (3 * i + j) + 8, :] = (
                shear_modulus * F[i][j] + factor * cof[i][j] + pulled * fiber[j]
            )
    nodal_ref[...] = dot(derivt_ref[...], work_ref[...], lax.Precision.HIGHEST)

    def deposit(turn, total):
        for pair in [turn * DEPOSIT + u for u in range(DEPOSIT)]:
            rows = nodal_ref[pl.ds(pl.multiple_of(8 * pair, 8), 8), :]
            for s in range(2):
                row = connect(2 * pair + s)
                value = both_halves(rows, s == 1)
                tail = value - value.astype(BF16).astype(F32)
                left = jnp.concatenate([spread_rows(value, row), spread_rows(tail, row)], axis=0)
                both_parts = dot_nt(left, node_onehot(row))
                total = total + both_parts[:128] + both_parts[128:]
        return total

    elastic_ref[...] = lax.fori_loop(0, 14 // DEPOSIT, deposit, jnp.zeros((128, 128), F32))


def share_row(share_ref, t):
    return jnp.concatenate([share_ref[4 * t + u : 4 * t + u + 1, :] for u in range(4)], axis=1)


def share_forces(elastic_ref, share_ref, shared_ref, turn_ref):
    sent = elastic_ref[...].astype(BF16)
    turn_ref[...] = jnp.zeros((128, 128), F32)
    for t in range(4):
        row = share_row(share_ref, t)
        picked = pick_rows(dot(sent, node_onehot(row)), row)
        for jj in range(4):
            turn_ref[16 * t + 4 * jj : 16 * t + 4 * jj + 4, :] = picked[0:4, 128 * jj : 128 * jj + 128]
    shared_ref[...] = turn_ref[...].T


def take_plane(rows_ref, q, stride):
    pieces = [rows_ref[pl.ds(3 * j + q, 128, stride=stride), :] for j in range(4)]
    return jnp.concatenate(pieces, axis=0).astype(BF16)


def put_plane(rows_ref, q, stride, plane):
    for j in range(4):
        rows_ref[pl.ds(3 * j + q, 128, stride=stride), :] = plane[128 * j : 128 * j + 128]


def couple_kernel(
    windex_ref, recv_ref, vel_ref, pick_ref, pickt_ref, table_ref, shared_ref,
    payload_ref, coupling_ref, rows_ref, chosen_ref, spread_ref, buffer_ref, sems,
):
    for g in range(8):
        for s in range(4):
            for k in range(4):
                pltpu.make_async_copy(
                    table_ref.at[windex_ref[k, 4 * g + s]],
                    buffer_ref.at[16 * g + 4 * s + k],
                    sems.at[g],
                ).start()
    rows_ref[0:1536, :] = recv_ref[...].astype(F32)
    chosen_ref[...] = jnp.zeros((512, 128), F32)
    pick = pick_ref[...]
    for q in range(3):
        chosen_ref[pl.ds(q, 128, stride=4), :] = dot(pick, take_plane(rows_ref, q, 12))

    def group(g, carry):
        part = pl.ds(pl.multiple_of(16 * g, 16), 16)
        pltpu.make_async_copy(table_ref.at[pl.ds(0, 16)], buffer_ref.at[part], sems.at[g]).wait()
        start = pl.multiple_of(16 * g, 16)
        left = jnp.concatenate(
            [chosen_ref[pl.ds(128 * k + start, 16), :] for k in range(4)], axis=1
        ).astype(BF16)
        owner = lax.broadcasted_iota(jnp.int32, (16, 128), 0) >> 2
        weights = []
        sampled = jnp.zeros((16, 128), F32)
        for s in range(4):
            weight = jnp.concatenate(
                [buffer_ref[16 * g + 4 * s + k] for k in range(4)], axis=1
            )
            weights.append(weight)
            sampled = jnp.where(owner == s, dot_nt(left, weight), sampled)
        coupling = penalty * (sampled - vel_ref[pl.ds(start, 16), :])
        coupling_ref[pl.ds(start, 16), :] = coupling
        pushed = (-coupling).astype(BF16)
        wide_owner = lax.broadcasted_iota(jnp.int32, (16, 512), 0) >> 2
        out = jnp.zeros((16, 512), F32)
        for s in range(4):
            out = jnp.where(wide_owner == s, dot(pushed, weights[s]), out)
        for k in range(4):
            spread_ref[pl.ds(128 * k + start, 16), :] = out[:, 128 * k : 128 * k + 128]
        return carry

    def groups(turn, carry):
        for u in range(GROUP):
            group(turn * GROUP + u, carry)
        return carry

    lax.fori_loop(0, 8 // GROUP, groups, 0)
    pickt = pickt_ref[...]
    for q in range(3):
        head, tail = split(spread_ref[pl.ds(q, 128, stride=4), :])
        put_plane(rows_ref, q, 14, dot(pickt, jnp.concatenate([head, tail], axis=0)))
    rows_ref[pl.ds(12, 128, stride=14), :] = shared_ref[...]
    rows_ref[pl.ds(13, 128, stride=14), :] = jnp.zeros((128, 128), F32)
    payload_ref[...] = rows_ref[...].astype(BF16)


def write_payload(send, blocks_ref, rows_ref, payload_ref):
    sent = dot(send, blocks_ref[...])
    for q in range(3):
        put_plane(rows_ref, q, 12, sent[:, 128 * q : 128 * q + 128])
    payload_ref[...] = rows_ref[0:1536, :].astype(BF16)


def store_blocks(blocks_ref, x, q, plane):
    for half in range(2):
        blocks_ref[128 * half + 16 * x : 128 * half + 16 * x + 16, 128 * q : 128 * q + 128] = plane[
            :, 128 * half : 128 * half + 128
        ].astype(BF16)


def pack_kernel(state_ref, send_ref, payload_ref, blocks_ref, rows_ref):
    for q in range(3):
        for x in range(8):
            store_blocks(blocks_ref, x, q, state_ref[q, x])
    write_payload(send_ref[...], blocks_ref, rows_ref, payload_ref)


def update_kernel(last):
    def kernel(
        recv_ref, state_ref, xlow_ref, xhigh_ref, ylow_ref, yhigh_ref, sendt_ref, send_ref,
        elastic_ref, coupling_ref, vel_ref, disp_ref, share_ref, *rest,
    ):
        if last:
            new_ref, velout_ref, dispout_ref, rows_ref, force_ref, turn_ref = rest
        else:
            (
                new_ref, velout_ref, dispout_ref, payload_ref, xlowout_ref, xhighout_ref,
                ylowout_ref, yhighout_ref, rows_ref, force_ref, turn_ref, blocks_ref,
            ) = rest
        rows_ref[...] = recv_ref[...].astype(F32)
        planes = jnp.concatenate(
            [take_plane(rows_ref, q, 14) for q in range(3)], axis=1
        )
        force_ref[...] = dot(sendt_ref[...], planes)

        turn_ref[...] = rows_ref[pl.ds(12, 128, stride=14), :].T
        total = elastic_ref[...]
        for t in range(4):
            row = share_row(share_ref, t)
            pieces = []
            for jj in range(4):
                first = 16 * t + 8 * (jj // 2)
                pieces.append(both_halves(turn_ref[first : first + 8, :], jj % 2 == 1))
            left = spread_rows(jnp.concatenate(pieces, axis=1), row)
            total = total + dot_nt(left, node_onehot(row))
        velocity = vel_ref[...] + time_step / node_mass * (total + coupling_ref[...])
        displace = disp_ref[...] + time_step * velocity
        if last:
            for h in range(32):
                velout_ref[h] = velocity[4 * h : 4 * h + 3]
                dispout_ref[h] = displace[4 * h : 4 * h + 3]
        else:
            velout_ref[...] = velocity
            dispout_ref[...] = displace

        yrow = lax.broadcasted_iota(jnp.int32, (16, 256), 0)
        zlane = lax.broadcasted_iota(jnp.int32, (16, 256), 1)

        def around(f, x):
            centre = state_ref[f, x]
            xm = xlow_ref[f] if x == 0 else state_ref[f, x - 1]
            xp = xhigh_ref[f] if x == 7 else state_ref[f, x + 1]
            ym = jnp.where(yrow == 0, ylow_ref[f, x], pltpu.roll(centre, 1, 0))
            yp = jnp.where(yrow == 15, yhigh_ref[f, x], pltpu.roll(centre, 15, 0))
            zm = jnp.where(zlane == 0, 0.0, pltpu.roll(centre, 1, 1))
            zp = jnp.where(zlane == 255, 0.0, pltpu.roll(centre, 255, 1))
            return centre, ((xm, xp), (ym, yp), (zm, zp))

        for x in range(8):
            density, near = around(3, x)
            divergence = jnp.zeros((16, 256), F32)
            for q in range(3):
                centre, pairs = around(q, x)
                laplace = -6.0 * centre
                for below, above in pairs:
                    laplace = laplace + (below + above)
                gradient = 0.5 * (near[q][1] - near[q][0])
                below, above = pairs[q]
                divergence = divergence + 0.5 * (
                    (1.0 + near[q][1]) * above - (1.0 + near[q][0]) * below
                )
                force = jnp.concatenate(
                    [
                        force_ref[128 * h + 16 * x : 128 * h + 16 * x + 16, 128 * q : 128 * q + 128]
                        for h in range(2)
                    ],
                    axis=1,
                )
                fresh = centre + time_step * (
                    viscosity * laplace - sound_square * gradient + force
                )
                new_ref[q, x] = fresh
                if not last:
                    store_blocks(blocks_ref, x, q, fresh)
                    put_edges(q, x, fresh, xlowout_ref, xhighout_ref, ylowout_ref, yhighout_ref)
            fresh = density - time_step * divergence
            new_ref[3, x] = fresh
            if not last:
                put_edges(3, x, fresh, xlowout_ref, xhighout_ref, ylowout_ref, yhighout_ref)
        if not last:
            write_payload(send_ref[...], blocks_ref, rows_ref, payload_ref)

    return kernel


def put_edges(f, x, fresh, xlowout_ref, xhighout_ref, ylowout_ref, yhighout_ref):
    if x == 0:
        xlowout_ref[f] = fresh
    if x == 7:
        xhighout_ref[f] = fresh
    ylowout_ref[f, x] = fresh[0:1]
    yhighout_ref[f, x] = fresh[15:16]


VMEM = pl.BlockSpec(memory_space=pltpu.VMEM)
SMEM = pl.BlockSpec(memory_space=pltpu.SMEM)
HBM = pl.BlockSpec(memory_space=pltpu.HBM)


def far(array):
    return pltpu.with_memory_space_constraint(array, pltpu.HBM)


def shape(dims, dtype=F32):
    return jax.ShapeDtypeStruct(dims, dtype)


def call(kernel, outs, specs, scratch, flops, mebibytes, out_specs=None):
    return pl.pallas_call(
        kernel,
        out_shape=outs,
        in_specs=specs,
        out_specs=out_specs or [VMEM] * len(outs),
        scratch_shapes=scratch,
        cost_estimate=pl.CostEstimate(flops=flops, transcendentals=0, bytes_accessed=2_000_000),
        compiler_params=pltpu.CompilerParams(vmem_limit_bytes=mebibytes * 1024 * 1024),
    )


def elastic_call(first):
    outs = [shape((128, 128))] * 2
    out_specs = [VMEM] * 2
    specs = [VMEM] * 6
    scratch = [
        pltpu.VMEM((112, 512), F32), pltpu.VMEM((72, 512), F32), pltpu.VMEM((128, 128), F32)
    ]
    if first:
        specs = [HBM] * 5
        scratch = scratch + [
            pltpu.VMEM((32, 3, 128), F32),
            pltpu.VMEM((32, 3, 128), F32),
            pltpu.VMEM((27, 512), jnp.int32),
            pltpu.VMEM((16, 128), jnp.int32),
            pltpu.VMEM((2, 512), F32),
            pltpu.SemaphoreType.DMA((5,)),
        ]
        out_specs = out_specs + [VMEM] * 5
        outs = outs + [shape((128, 128))] * 2
        outs = outs + [shape((72, 112)), shape((112, 72)), shape((3, 512))]
    return call(elastic_kernel(first), outs, specs, scratch, 3_000_000_000, 16, out_specs)


def couple_call():
    return call(
        couple_kernel,
        [shape((1792, 128), BF16), shape((128, 128))],
        [SMEM] + [VMEM] * 4 + [HBM, VMEM],
        [
            pltpu.VMEM((1792, 128), F32),
            pltpu.VMEM((512, 128), F32),
            pltpu.VMEM((512, 128), F32),
            pltpu.VMEM((128, 128, 128), BF16),
            pltpu.SemaphoreType.DMA((8,)),
        ],
        1_000_000_000,
        24,
    )


def pack_call():
    return call(
        pack_kernel,
        [shape((1536, 128), BF16)],
        [VMEM] * 2,
        [pltpu.VMEM((256, 384), BF16), pltpu.VMEM((1792, 128), F32)],
        200_000_000,
        16,
    )


def update_call(last):
    nodes = shape((32, 3, 128)) if last else shape((128, 128))
    outs = [shape((4, 8, 16, 256)), nodes, nodes]
    scratch = [
        pltpu.VMEM((1792, 128), F32),
        pltpu.VMEM((256, 384), F32),
        pltpu.VMEM((128, 128), F32),
    ]
    if not last:
        outs = outs + [
            shape((1536, 128), BF16),
            shape((4, 16, 256)),
            shape((4, 16, 256)),
            shape((4, 8, 1, 256)),
            shape((4, 8, 1, 256)),
        ]
        scratch = scratch + [pltpu.VMEM((256, 384), BF16)]
    return call(
        update_kernel(last), outs, [VMEM] * 13, scratch, 500_000_000,
        16,
    )


def exchange(payload, dims):
    moved = lax.all_to_all(
        payload.reshape((128,) + dims + (128,)), AXES, split_axis=0, concat_axis=0, tiled=True
    )
    return moved.reshape(-1, 128)


def halo(edges):
    xlow, xhigh, ylow, yhigh = edges

    def shift(low, high, axis):
        size = lax.axis_size(axis)
        up = [(i, i + 1) for i in range(size - 1)]
        down = [(b, a) for a, b in up]
        return lax.ppermute(high, axis, up), lax.ppermute(low, axis, down)

    xm, xp = shift(xlow, xhigh, "gx")
    ym, yp = shift(ylow, yhigh, "gy")
    return xm, xp, ym, yp


def body(
    fluid_state, node_disp, node_vel, fiber_angles, connectivity,
    send_blocks, interp_slots, weight_index, share_nodes, weight_table,
):
    share = share_nodes[0].T
    sends = send_blocks[0].T
    sends = jnp.where(sends < 256, (sends & 1) * 128 + (sends >> 1), -1)
    blocks_range = jnp.arange(256, dtype=jnp.int32)
    slots_range = jnp.arange(512, dtype=jnp.int32)
    send = (sends[:, :, None] == blocks_range[None, None, :]).astype(BF16).reshape(512, 256)
    sendt = (blocks_range[:, None] == sends.reshape(512)[None, :]).astype(BF16)
    slots = (interp_slots & 3) * 128 + (interp_slots >> 2)
    pick = (slots[:, :, None] == slots_range[None, None, :]).astype(BF16).reshape(128, 512)
    flat = slots.reshape(128)
    pickt = (slots_range[:, None] == jnp.concatenate([flat, flat])[None, :]).astype(BF16)

    state = fluid_state
    payload = pack_call()(state, send)[0]
    edges = (state[:, 0], state[:, 7], state[:, :, 0:1], state[:, :, 15:16])
    start_disp = node_disp.reshape(3, 32, 128).transpose(1, 0, 2)
    start_vel = node_vel.reshape(3, 32, 128).transpose(1, 0, 2)
    for step in range(STEPS):
        last = step == STEPS - 1
        received = exchange(payload, (3, 4))
        around = halo(edges)
        if step == 0:
            elastic, shared, displace, velocity, *tables = elastic_call(True)(
                *map(far, (start_disp, start_vel, connectivity, share, fiber_angles))
            )
        else:
            elastic, shared = elastic_call(False)(displace, connectivity, share, *tables)
        outbound, coupling = couple_call()(
            far(weight_index), received, velocity, pick, pickt, far(weight_table), shared
        )
        inbound = exchange(outbound, (7, 2))
        results = update_call(last)(
            inbound, state, *around, sendt, send, elastic, coupling, velocity, displace, share
        )
        state, velocity, displace = results[:3]
        if not last:
            payload = results[3]
            edges = results[4:8]
    out = [nodes.transpose(1, 0, 2).reshape(3, 4096) for nodes in (displace, velocity)]
    return (state, out[0], out[1])


def solution(mesh):
    placed = (
        P(None, "gx", "gy", None),
        P(None, AXES),
        P(None, AXES),
        P(None, AXES),
        P(None, AXES),
        P(AXES, None, None),
        P(None, AXES),
        P(None, AXES),
        P(AXES, None, None),
        P(),
    )
    return jax.shard_map(
        body,
        mesh=mesh,
        in_specs=placed,
        out_specs=(P(None, "gx", "gy", None), P(None, AXES), P(None, AXES)),
        check_vma=False,
    )
```

```python
import math

import jax
import jax.numpy as jnp
from jax import lax
from jax.experimental import pallas as pl
from jax.experimental.pallas import tpu as pltpu
from jax.sharding import PartitionSpec as P


STEPS = 3

time_step = 0.1
viscosity = 1.0
sound_square = 1.0
penalty = 4.0
node_mass = 0.5
shear_modulus = 2.0
bulk_modulus = 4.0
fiber_stiff = 2.0
fiber_exponent = 1.0

BF16 = jnp.bfloat16
F32 = jnp.float32
AXES = ("gx", "gy")
FETCH = 7
DEPOSIT = 7
GROUP = 8


def lagrange(degree, position):
    outer = 0.5 * position * position
    ends = jnp.where(degree == 0, outer - 0.5 * position, outer + 0.5 * position)
    return jnp.where(degree == 1, 1.0 - position * position, ends)


def slope(degree, position):
    ends = jnp.where(degree == 0, position - 0.5, position + 0.5)
    return jnp.where(degree == 1, -2.0 * position, ends)


def derivative_matrix(dims, row_axis):
    row = lax.broadcasted_iota(jnp.int32, dims, row_axis)
    column = lax.broadcasted_iota(jnp.int32, dims, 1 - row_axis)
    i = (row * 171) >> 12
    j = (row - 24 * i) >> 3
    point = row & 7
    node = column >> 2
    first = (node * 57) >> 9
    middle = (node * 43) >> 7
    orders = (first, middle - 3 * first, node - 3 * middle)
    coords = (point >> 2, (point >> 1) & 1, point & 1)
    value = jnp.where(((column & 3) == i) & (node < 27), 2.0, 0.0)
    for axis in range(3):
        position = jnp.where(coords[axis] == 0, -1.0 / math.sqrt(3.0), 1.0 / math.sqrt(3.0))
        value = value * jnp.where(
            j == axis, slope(orders[axis], position), lagrange(orders[axis], position)
        )
    return value


def dot(a, b, precision=None):
    return lax.dot_general(
        a, b, (((1,), (0,)), ((), ())), precision=precision, preferred_element_type=F32
    )


def dot_nt(a, b):
    return lax.dot_general(a, b, (((1,), (1,)), ((), ())), preferred_element_type=F32)


def packed_offset(values, shift):
    rows = lax.broadcasted_iota(jnp.int32, (16, 512), 0) >> shift
    return (jnp.broadcast_to(values, (16, 512)) - rows).astype(F32).astype(BF16)


def node_onehot(row):
    offset = packed_offset(row & 127, 0)
    one, zero = jnp.ones((16, 512), BF16), jnp.zeros((16, 512), BF16)
    return jnp.concatenate(
        [jnp.where(offset == jnp.asarray(16 * r, BF16), one, zero) for r in range(8)], axis=0
    )


def pick_rows(table, row):
    high = jnp.broadcast_to(row >> 7, (8, 512)) - (
        lax.broadcasted_iota(jnp.int32, (8, 512), 0) >> 2
    )
    picked = jnp.where(high == 0, table[0:8], 0.0)
    for r in range(1, 16):
        picked = jnp.where(high == 2 * r, table[8 * r : 8 * r + 8], picked)
    return picked + pltpu.roll(picked, 4, 0)


def spread_rows(value, row):
    high = packed_offset(row >> 7, 2)
    wide = jnp.concatenate([value, value], axis=0).astype(BF16)
    zero = jnp.zeros((16, 512), BF16)
    return jnp.concatenate(
        [jnp.where(high == jnp.asarray(4 * r, BF16), wide, zero) for r in range(8)], axis=0
    )


def both_halves(value, odd):
    turned = pltpu.roll(value, 4, 0)
    low = lax.broadcasted_iota(jnp.int32, value.shape, 0) < 4
    return jnp.where(low, turned, value) if odd else jnp.where(low, value, turned)


def split(value):
    head = value.astype(BF16)
    return head, (value - head.astype(F32)).astype(BF16)


def elastic_kernel(first):
    def kernel(*refs):
        if first:
            (
                elastic_ref, shared_ref, rows_ref, velrows_ref, deriv_ref, derivt_ref, fiber_ref,
            ) = refs[5:12]
            nodal_ref, work_ref, turn_ref = refs[12:15]
            loaded, sems = refs[15:20], refs[20]
            loads = [pltpu.make_async_copy(refs[n], loaded[n], sems.at[n]) for n in range(5)]
            for load in loads:
                load.start()
            disp_ref, vel_ref, conn_ref, share_ref, angle_ref = loaded
            for load in loads:
                load.wait()
            rows_ref[...] = jnp.zeros((128, 128), F32)
            velrows_ref[...] = jnp.zeros((128, 128), F32)
            for h in range(32):
                rows_ref[4 * h : 4 * h + 3, :] = disp_ref[h]
                velrows_ref[4 * h : 4 * h + 3, :] = vel_ref[h]
            deriv_ref[...] = derivative_matrix((72, 112), 0)
            derivt_ref[...] = -0.125 * derivative_matrix((112, 72), 1)
            angles = angle_ref[...]
            cosine, sine = jnp.cos(angles), jnp.sin(angles)
            fiber_ref[0:1, :] = cosine[0:1] * cosine[1:2]
            fiber_ref[1:2, :] = cosine[0:1] * sine[1:2]
            fiber_ref[2:3, :] = sine[0:1]
        else:
            rows_ref, conn_ref, share_ref, deriv_ref, derivt_ref, fiber_ref = refs[:6]
            elastic_ref, shared_ref, nodal_ref, work_ref, turn_ref = refs[6:]
        elastic_forces(
            rows_ref, conn_ref, deriv_ref, derivt_ref, fiber_ref, elastic_ref, nodal_ref, work_ref
        )
        share_forces(elastic_ref, share_ref, shared_ref, turn_ref)

    return kernel


def elastic_forces(
    disp_ref, conn_ref, deriv_ref, derivt_ref, fiber_ref, elastic_ref, nodal_ref, work_ref
):
    head, tail = split(disp_ref[...])
    both = jnp.concatenate([head, tail], axis=1)

    def connect(node):
        return conn_ref[pl.ds(jnp.minimum(node, 26), 1), :]

    def fetch(turn, carry):
        for pair in [turn * FETCH + u for u in range(FETCH)]:
            halves = []
            for s in range(2):
                row = connect(2 * pair + s)
                hot = node_onehot(row)
                table = dot(both, jnp.concatenate([hot, hot], axis=0))
                halves.append(pick_rows(table, row))
            low = lax.broadcasted_iota(jnp.int32, (8, 512), 0) < 4
            nodal_ref[pl.ds(pl.multiple_of(8 * pair, 8), 8), :] = jnp.where(
                low, halves[0], halves[1]
            )
        return carry

    lax.fori_loop(0, 14 // FETCH, fetch, 0)
    work_ref[...] = dot(deriv_ref[...], nodal_ref[...], lax.Precision.HIGHEST)

    def entry(i, j):
        value = work_ref[8 * (3 * i + j) : 8 * (3 * i + j) + 8, :]
        return value + 1.0 if i == j else value

    F = [[entry(i, j) for j in range(3)] for i in range(3)]
    fiber = [fiber_ref[j : j + 1, :] for j in range(3)]

    def cofactor(i, j):
        i1, i2, j1, j2 = (i + 1) % 3, (i + 2) % 3, (j + 1) % 3, (j + 2) % 3
        return F[i1][j1] * F[i2][j2] - F[i1][j2] * F[i2][j1]

    cof = [[cofactor(i, j) for j in range(3)] for i in range(3)]
    volume = F[0][0] * cof[0][0] + F[0][1] * cof[0][1] + F[0][2] * cof[0][2]
    along = [F[i][0] * fiber[0] + F[i][1] * fiber[1] + F[i][2] * fiber[2] for i in range(3)]
    excess = along[0] * along[0] + along[1] * along[1] + along[2] * along[2] - 1.0
    weight = 2.0 * fiber_stiff * excess * jnp.exp(fiber_exponent * excess * excess)
    factor = bulk_modulus * (volume - 1.0) - shear_modulus
    for i in range(3):
        pulled = weight * along[i]
        for j in range(3):
            work_ref[8 * (3 * i + j) : 8 * (3 * i + j) + 8, :] = (
                shear_modulus * F[i][j] + factor * cof[i][j] + pulled * fiber[j]
            )
    nodal_ref[...] = dot(derivt_ref[...], work_ref[...], lax.Precision.HIGHEST)

    def deposit(turn, total):
        for pair in [turn * DEPOSIT + u for u in range(DEPOSIT)]:
            rows = nodal_ref[pl.ds(pl.multiple_of(8 * pair, 8), 8), :]
            for s in range(2):
                row = connect(2 * pair + s)
                value = both_halves(rows, s == 1)
                tail = value - value.astype(BF16).astype(F32)
                left = jnp.concatenate([spread_rows(value, row), spread_rows(tail, row)], axis=0)
                both_parts = dot_nt(left, node_onehot(row))
                total = total + both_parts[:128] + both_parts[128:]
        return total

    elastic_ref[...] = lax.fori_loop(0, 14 // DEPOSIT, deposit, jnp.zeros((128, 128), F32))


def share_row(share_ref, t):
    return jnp.concatenate([share_ref[4 * t + u : 4 * t + u + 1, :] for u in range(4)], axis=1)


def share_forces(elastic_ref, share_ref, shared_ref, turn_ref):
    sent = elastic_ref[...].astype(BF16)
    turn_ref[...] = jnp.zeros((128, 128), F32)
    for t in range(4):
        row = share_row(share_ref, t)
        picked = pick_rows(dot(sent, node_onehot(row)), row)
        for jj in range(4):
            turn_ref[16 * t + 4 * jj : 16 * t + 4 * jj + 4, :] = picked[0:4, 128 * jj : 128 * jj + 128]
    shared_ref[...] = turn_ref[...].T


def take_plane(rows_ref, q, stride):
    pieces = [rows_ref[pl.ds(3 * j + q, 128, stride=stride), :] for j in range(4)]
    return jnp.concatenate(pieces, axis=0).astype(BF16)


def put_plane(rows_ref, q, stride, plane):
    for j in range(4):
        rows_ref[pl.ds(3 * j + q, 128, stride=stride), :] = plane[128 * j : 128 * j + 128]


def couple_kernel(
    windex_ref, recv_ref, vel_ref, pick_ref, pickt_ref, table_ref, shared_ref,
    payload_ref, coupling_ref, rows_ref, chosen_ref, spread_ref, buffer_ref, sems,
):
    for g in range(8):
        for s in range(4):
            for k in range(4):
                pltpu.make_async_copy(
                    table_ref.at[windex_ref[k, 4 * g + s]],
                    buffer_ref.at[16 * g + 4 * s + k],
                    sems.at[g],
                ).start()
    rows_ref[0:1536, :] = recv_ref[...].astype(F32)
    chosen_ref[...] = jnp.zeros((512, 128), F32)
    pick = pick_ref[...]
    for q in range(3):
        chosen_ref[pl.ds(q, 128, stride=4), :] = dot(pick, take_plane(rows_ref, q, 12))

    def group(g, carry):
        part = pl.ds(pl.multiple_of(16 * g, 16), 16)
        pltpu.make_async_copy(table_ref.at[pl.ds(0, 16)], buffer_ref.at[part], sems.at[g]).wait()
        start = pl.multiple_of(16 * g, 16)
        left = jnp.concatenate(
            [chosen_ref[pl.ds(128 * k + start, 16), :] for k in range(4)], axis=1
        ).astype(BF16)
        owner = lax.broadcasted_iota(jnp.int32, (16, 128), 0) >> 2
        weights = []
        sampled = jnp.zeros((16, 128), F32)
        for s in range(4):
            weight = jnp.concatenate(
                [buffer_ref[16 * g + 4 * s + k] for k in range(4)], axis=1
            )
            weights.append(weight)
            sampled = jnp.where(owner == s, dot_nt(left, weight), sampled)
        coupling = penalty * (sampled - vel_ref[pl.ds(start, 16), :])
        coupling_ref[pl.ds(start, 16), :] = coupling
        pushed = (-coupling).astype(BF16)
        wide_owner = lax.broadcasted_iota(jnp.int32, (16, 512), 0) >> 2
        out = jnp.zeros((16, 512), F32)
        for s in range(4):
            out = jnp.where(wide_owner == s, dot(pushed, weights[s]), out)
        for k in range(4):
            spread_ref[pl.ds(128 * k + start, 16), :] = out[:, 128 * k : 128 * k + 128]
        return carry

    def groups(turn, carry):
        for u in range(GROUP):
            group(turn * GROUP + u, carry)
        return carry

    lax.fori_loop(0, 8 // GROUP, groups, 0)
    pickt = pickt_ref[...]
    for q in range(3):
        head, tail = split(spread_ref[pl.ds(q, 128, stride=4), :])
        put_plane(rows_ref, q, 14, dot(pickt, jnp.concatenate([head, tail], axis=0)))
    rows_ref[pl.ds(12, 128, stride=14), :] = shared_ref[...]
    rows_ref[pl.ds(13, 128, stride=14), :] = jnp.zeros((128, 128), F32)
    payload_ref[...] = rows_ref[...].astype(BF16)


def write_payload(send, blocks_ref, rows_ref, payload_ref):
    sent = dot(send, blocks_ref[...])
    for q in range(3):
        put_plane(rows_ref, q, 12, sent[:, 128 * q : 128 * q + 128])
    payload_ref[...] = rows_ref[0:1536, :].astype(BF16)


def store_blocks(blocks_ref, x, q, plane):
    for half in range(2):
        blocks_ref[128 * half + 16 * x : 128 * half + 16 * x + 16, 128 * q : 128 * q + 128] = plane[
            :, 128 * half : 128 * half + 128
        ].astype(BF16)


def pack_kernel(
    state_ref, send_ref, payload_ref, xlow_ref, xhigh_ref, ylow_ref, yhigh_ref, blocks_ref, rows_ref
):
    for f in range(4):
        for x in range(8):
            plane = state_ref[f, x]
            if f < 3:
                store_blocks(blocks_ref, x, f, plane)
            put_edges(f, x, plane, xlow_ref, xhigh_ref, ylow_ref, yhigh_ref)
    write_payload(send_ref[...], blocks_ref, rows_ref, payload_ref)


def update_kernel(last):
    def kernel(
        recv_ref, state_ref, xlow_ref, xhigh_ref, ylow_ref, yhigh_ref, sendt_ref, send_ref,
        elastic_ref, coupling_ref, vel_ref, disp_ref, share_ref, *rest,
    ):
        if last:
            new_ref, velout_ref, dispout_ref, rows_ref, force_ref, turn_ref = rest
        else:
            (
                new_ref, velout_ref, dispout_ref, payload_ref, xlowout_ref, xhighout_ref,
                ylowout_ref, yhighout_ref, rows_ref, force_ref, turn_ref, blocks_ref,
            ) = rest
        rows_ref[...] = recv_ref[...].astype(F32)
        planes = jnp.concatenate(
            [take_plane(rows_ref, q, 14) for q in range(3)], axis=1
        )
        force_ref[...] = dot(sendt_ref[...], planes)

        turn_ref[...] = rows_ref[pl.ds(12, 128, stride=14), :].T
        total = elastic_ref[...]
        for t in range(4):
            row = share_row(share_ref, t)
            pieces = []
            for jj in range(4):
                first = 16 * t + 8 * (jj // 2)
                pieces.append(both_halves(turn_ref[first : first + 8, :], jj % 2 == 1))
            left = spread_rows(jnp.concatenate(pieces, axis=1), row)
            total = total + dot_nt(left, node_onehot(row))
        velocity = vel_ref[...] + time_step / node_mass * (total + coupling_ref[...])
        displace = disp_ref[...] + time_step * velocity
        if last:
            for h in range(32):
                velout_ref[h] = velocity[4 * h : 4 * h + 3]
                dispout_ref[h] = displace[4 * h : 4 * h + 3]
        else:
            velout_ref[...] = velocity
            dispout_ref[...] = displace

        yrow = lax.broadcasted_iota(jnp.int32, (16, 256), 0)
        zlane = lax.broadcasted_iota(jnp.int32, (16, 256), 1)

        def around(f, x):
            centre = state_ref[f, x]
            xm = xlow_ref[f].astype(F32) if x == 0 else state_ref[f, x - 1]
            xp = xhigh_ref[f].astype(F32) if x == 7 else state_ref[f, x + 1]
            ym = jnp.where(yrow == 0, ylow_ref[f, x], pltpu.roll(centre, 1, 0))
            yp = jnp.where(yrow == 15, yhigh_ref[f, x], pltpu.roll(centre, 15, 0))
            zm = jnp.where(zlane == 0, 0.0, pltpu.roll(centre, 1, 1))
            zp = jnp.where(zlane == 255, 0.0, pltpu.roll(centre, 255, 1))
            return centre, ((xm, xp), (ym, yp), (zm, zp))

        for x in range(8):
            density, near = around(3, x)
            divergence = jnp.zeros((16, 256), F32)
            for q in range(3):
                centre, pairs = around(q, x)
                laplace = -6.0 * centre
                for below, above in pairs:
                    laplace = laplace + (below + above)
                gradient = 0.5 * (near[q][1] - near[q][0])
                below, above = pairs[q]
                divergence = divergence + 0.5 * (
                    (1.0 + near[q][1]) * above - (1.0 + near[q][0]) * below
                )
                force = jnp.concatenate(
                    [
                        force_ref[128 * h + 16 * x : 128 * h + 16 * x + 16, 128 * q : 128 * q + 128]
                        for h in range(2)
                    ],
                    axis=1,
                )
                fresh = centre + time_step * (
                    viscosity * laplace - sound_square * gradient + force
                )
                new_ref[q, x] = fresh
                if not last:
                    store_blocks(blocks_ref, x, q, fresh)
                    put_edges(q, x, fresh, xlowout_ref, xhighout_ref, ylowout_ref, yhighout_ref)
            fresh = density - time_step * divergence
            new_ref[3, x] = fresh
            if not last:
                put_edges(3, x, fresh, xlowout_ref, xhighout_ref, ylowout_ref, yhighout_ref)
        if not last:
            write_payload(send_ref[...], blocks_ref, rows_ref, payload_ref)

    return kernel


def put_edges(f, x, fresh, xlowout_ref, xhighout_ref, ylowout_ref, yhighout_ref):
    if x == 0:
        xlowout_ref[f] = fresh.astype(BF16)
    if x == 7:
        xhighout_ref[f] = fresh.astype(BF16)
    ylowout_ref[f, x] = fresh[0:1]
    yhighout_ref[f, x] = fresh[15:16]


VMEM = pl.BlockSpec(memory_space=pltpu.VMEM)
SMEM = pl.BlockSpec(memory_space=pltpu.SMEM)
HBM = pl.BlockSpec(memory_space=pltpu.HBM)


def far(array):
    return pltpu.with_memory_space_constraint(array, pltpu.HBM)


def shape(dims, dtype=F32):
    return jax.ShapeDtypeStruct(dims, dtype)


EDGES = [shape((4, 16, 256), BF16)] * 2 + [shape((4, 8, 1, 256))] * 2


def call(kernel, outs, specs, scratch, flops, mebibytes, out_specs=None):
    return pl.pallas_call(
        kernel,
        out_shape=outs,
        in_specs=specs,
        out_specs=out_specs or [VMEM] * len(outs),
        scratch_shapes=scratch,
        cost_estimate=pl.CostEstimate(flops=flops, transcendentals=0, bytes_accessed=2_000_000),
        compiler_params=pltpu.CompilerParams(vmem_limit_bytes=mebibytes * 1024 * 1024),
    )


def elastic_call(first):
    outs = [shape((128, 128))] * 2
    out_specs = [VMEM] * 2
    specs = [VMEM] * 6
    scratch = [
        pltpu.VMEM((112, 512), F32), pltpu.VMEM((72, 512), F32), pltpu.VMEM((128, 128), F32)
    ]
    if first:
        specs = [HBM] * 5
        scratch = scratch + [
            pltpu.VMEM((32, 3, 128), F32),
            pltpu.VMEM((32, 3, 128), F32),
            pltpu.VMEM((27, 512), jnp.int32),
            pltpu.VMEM((16, 128), jnp.int32),
            pltpu.VMEM((2, 512), F32),
            pltpu.SemaphoreType.DMA((5,)),
        ]
        out_specs = out_specs + [VMEM] * 5
        outs = outs + [shape((128, 128))] * 2
        outs = outs + [shape((72, 112)), shape((112, 72)), shape((3, 512))]
    return call(elastic_kernel(first), outs, specs, scratch, 3_000_000_000, 16, out_specs)


def couple_call():
    return call(
        couple_kernel,
        [shape((1792, 128), BF16), shape((128, 128))],
        [SMEM] + [VMEM] * 4 + [HBM, VMEM],
        [
            pltpu.VMEM((1792, 128), F32),
            pltpu.VMEM((512, 128), F32),
            pltpu.VMEM((512, 128), F32),
            pltpu.VMEM((128, 128, 128), BF16),
            pltpu.SemaphoreType.DMA((8,)),
        ],
        1_000_000_000,
        24,
    )


def pack_call():
    return call(
        pack_kernel,
        [shape((1536, 128), BF16)] + EDGES,
        [VMEM] * 2,
        [pltpu.VMEM((256, 384), BF16), pltpu.VMEM((1792, 128), F32)],
        200_000_000,
        16,
    )


def update_call(last):
    nodes = shape((32, 3, 128)) if last else shape((128, 128))
    outs = [shape((4, 8, 16, 256)), nodes, nodes]
    scratch = [
        pltpu.VMEM((1792, 128), F32),
        pltpu.VMEM((256, 384), F32),
        pltpu.VMEM((128, 128), F32),
    ]
    if not last:
        outs = outs + [shape((1536, 128), BF16)] + EDGES
        scratch = scratch + [pltpu.VMEM((256, 384), BF16)]
    return call(
        update_kernel(last), outs, [VMEM] * 13, scratch, 500_000_000,
        16,
    )


def exchange(payload, dims):
    moved = lax.all_to_all(
        payload.reshape((128,) + dims + (128,)), AXES, split_axis=0, concat_axis=0, tiled=True
    )
    return moved.reshape(-1, 128)


def halo(edges):
    xlow, xhigh, ylow, yhigh = edges

    def shift(low, high, axis):
        size = lax.axis_size(axis)
        up = [(i, i + 1) for i in range(size - 1)]
        down = [(b, a) for a, b in up]
        return lax.ppermute(high, axis, up), lax.ppermute(low, axis, down)

    xm, xp = shift(xlow, xhigh, "gx")
    ym, yp = shift(ylow, yhigh, "gy")
    return xm, xp, ym, yp


def body(
    fluid_state, node_disp, node_vel, fiber_angles, connectivity,
    send_blocks, interp_slots, weight_index, share_nodes, weight_table,
):
    share = share_nodes[0].T
    sends = send_blocks[0].T
    sends = jnp.where(sends < 256, (sends & 1) * 128 + (sends >> 1), -1)
    blocks_range = jnp.arange(256, dtype=jnp.int32)
    slots_range = jnp.arange(512, dtype=jnp.int32)
    send = (sends[:, :, None] == blocks_range[None, None, :]).astype(BF16).reshape(512, 256)
    sendt = (blocks_range[:, None] == sends.reshape(512)[None, :]).astype(BF16)
    slots = (interp_slots & 3) * 128 + (interp_slots >> 2)
    pick = (slots[:, :, None] == slots_range[None, None, :]).astype(BF16).reshape(128, 512)
    flat = slots.reshape(128)
    pickt = (slots_range[:, None] == jnp.concatenate([flat, flat])[None, :]).astype(BF16)

    state = fluid_state
    payload, *edges = pack_call()(state, send)
    start_disp = node_disp.reshape(3, 32, 128).transpose(1, 0, 2)
    start_vel = node_vel.reshape(3, 32, 128).transpose(1, 0, 2)
    for step in range(STEPS):
        last = step == STEPS - 1
        received = exchange(payload, (3, 4))
        around = halo(edges)
        if step == 0:
            elastic, shared, displace, velocity, *tables = elastic_call(True)(
                *map(far, (start_disp, start_vel, connectivity, share, fiber_angles))
            )
        else:
            elastic, shared = elastic_call(False)(displace, connectivity, share, *tables)
        outbound, coupling = couple_call()(
            far(weight_index), received, velocity, pick, pickt, far(weight_table), shared
        )
        inbound = exchange(outbound, (7, 2))
        results = update_call(last)(
            inbound, state, *around, sendt, send, elastic, coupling, velocity, displace, share
        )
        state, velocity, displace = results[:3]
        if not last:
            payload = results[3]
            edges = results[4:8]
    out = [nodes.transpose(1, 0, 2).reshape(3, 4096) for nodes in (displace, velocity)]
    return (state, out[0], out[1])


def solution(mesh):
    placed = (
        P(None, "gx", "gy", None),
        P(None, AXES),
        P(None, AXES),
        P(None, AXES),
        P(None, AXES),
        P(AXES, None, None),
        P(None, AXES),
        P(None, AXES),
        P(AXES, None, None),
        P(),
    )
    return jax.shard_map(
        body,
        mesh=mesh,
        in_specs=placed,
        out_specs=(P(None, "gx", "gy", None), P(None, AXES), P(None, AXES)),
        check_vma=False,
    )
```
